32 devices in a mesh: seq: 4 (over z), uly: 4 (over y, x), rep: 2 (over core).
Axes of the slice: x: 2, y: 2, z: 4, core: 2. Of those that a mesh axis runs over, the one named last changes fastest.
Arguments:
- queries: bfloat16 [4096, 2048], P(('rep', 'seq', 'uly')), parts along dimension 0, may hold values from -6 to 6
- keys: bfloat16 [4096, 2048], P(('rep', 'seq', 'uly')), parts along dimension 0, may hold values from -6 to 6
- values: bfloat16 [4096, 2048], P(('rep', 'seq', 'uly')), parts along dimension 0, may hold values from -6 to 6
- past_outputs: bfloat16 [2, 4096, 2048], P(None, ('rep', 'seq', 'uly')), parts along dimension 1, may hold values from -6 to 6
- dwa_slot: int32 [2], replicated, may hold values from 0 to 63
- dwa_table: float32 [2, 64], replicated, may hold values from 0.1 to 0.6
Outputs:
- mixed: bfloat16 [4096, 2048], P(('rep', 'seq', 'uly')), parts along dimension 0
The draws below stay inside these ranges and needn't reach their ends.
There are 2 independent parts, one for each index of `rep`. The reference program is written for one: setup_inputs(seed, part) draws one part's arguments, and reference() takes and returns one part's arrays. A program takes and returns all parts, laid end to end along the dimension named above; an argument that names none is the same for every part. Nothing has to cross between parts.
All inputs are finite; a program needn't handle non-finite values.
Results may differ from the reference program's by a relative error of at most 0.0034.
Values may be sent and summed in bfloat16 or wider, within the bound.
A program may use at most 64 MiB of HBM per device.

```python
import jax
import jax.numpy as jnp
from jax import lax

HEADS = 16
HEAD_DIM = 128
PAST = 2
TABLE = 64
TOK_DEV = 128
SPAN = 4
TOKENS = 2048
N_SEQ = 4
N_ULY = 4


def drawn_pair(key):
    base = jax.random.fold_in(key, 7)
    width = HEADS * HEAD_DIM
    query_field = jnp.clip(2.5 * jax.random.normal(jax.random.fold_in(base, 1), (TOKENS, width), jnp.float32), -6.0, 6.0)
    key_field = jnp.clip(jax.random.normal(jax.random.fold_in(base, 2), (TOKENS, width), jnp.float32), -6.0, 6.0)
    return (query_field, key_field)


def draw_queries(key, part):
    return drawn_pair(key)[0].astype(jnp.bfloat16)


def draw_keys(key, part):
    return drawn_pair(key)[1].astype(jnp.bfloat16)


def block_levels(rng, shape, split, low, largest):
    factor_of, own = 1.0, jax.random.fold_in(rng, 6)
    for dim, shards_of in split:
        heights = jnp.exp(jax.random.uniform(jax.random.fold_in(own, dim), (shards_of,), jnp.float32, low / len(split), largest / len(split)))
        factor_of = factor_of * jnp.repeat(heights, shape[dim] // shards_of).reshape([-1 if axis == dim else 1 for axis in range(len(shape))])
    return factor_of


def scatter_about(stream_key, dims, spread, most, cuts=(), held_as=jnp.bfloat16):
    array = jax.random.normal(stream_key, dims, jnp.float32) * spread
    if len(cuts) > 0:
        array = block_levels(stream_key, dims, cuts, -0.22, 0.18) * array
    return jnp.clip(array, min=-most, max=most).astype(held_as)


def setup_inputs(seed: int = 0, part: int = 0) -> dict:
    key_list = jax.random.split(jax.random.key(seed), 7)
    part_keys = jax.random.split(jax.random.fold_in(key_list[6], part), 7)
    return {
        "queries": draw_queries(jax.random.fold_in(jax.random.fold_in(key_list[6], part), 71), part),
        "keys": draw_keys(jax.random.fold_in(jax.random.fold_in(key_list[6], part), 71), part),
        "values": scatter_about(part_keys[2], (TOKENS, HEADS * HEAD_DIM), 1.0, 6.0, ((0, 16),)),
        "past_outputs": scatter_about(part_keys[3], (PAST, TOKENS, HEADS * HEAD_DIM), 1.0, 6.0, ((1, 16),)),
        "dwa_slot": jax.random.randint(key_list[4], (PAST,), 0, TABLE).astype(jnp.int32),
        "dwa_table": jnp.clip(jax.random.uniform(key_list[5], (2, TABLE), jnp.float32, 0.1, 0.6), 0.1, 0.6),
    }


def one_head(items):
    query, key_block, value_block, allowed = items
    scores = jnp.dot(query, key_block.T, preferred_element_type=jnp.float32) * (1.0 / (HEAD_DIM ** 0.5))
    scores = jnp.where(allowed, scores, -jnp.inf)
    top_score = jnp.max(scores, axis=1, keepdims=True)
    prob = jnp.exp(scores - top_score)
    total = jnp.sum(prob, axis=1, keepdims=True)
    weights = prob.astype(jnp.bfloat16)
    summed = jnp.dot(weights, value_block, preferred_element_type=jnp.float32)
    return (summed / total).astype(jnp.bfloat16)


def reference(queries, keys, values, past_outputs, dwa_slot, dwa_table):
    block_rows = N_ULY * TOK_DEV

    def arrange(field):
        return field.reshape(N_SEQ, block_rows, HEADS, HEAD_DIM)

    padding = jnp.zeros((SPAN - 1, block_rows, HEADS, HEAD_DIM), jnp.bfloat16)
    query_all = arrange(queries)
    key_padded = jnp.concatenate([padding, arrange(keys)], axis=0)
    value_padded = jnp.concatenate([padding, arrange(values)], axis=0)

    def one_block(block):
        query_block = lax.dynamic_index_in_dim(query_all, block, 0, keepdims=False)
        key_window = lax.dynamic_slice_in_dim(key_padded, block, SPAN, 0).reshape(SPAN * block_rows, HEADS, HEAD_DIM)
        value_window = lax.dynamic_slice_in_dim(value_padded, block, SPAN, 0).reshape(SPAN * block_rows, HEADS, HEAD_DIM)
        query_pos = block * block_rows + jnp.arange(block_rows, dtype=jnp.int32)
        key_pos = (block - SPAN + 1) * block_rows + jnp.arange(SPAN * block_rows, dtype=jnp.int32)
        allowed = (key_pos[None, :] <= query_pos[:, None]) & (key_pos[None, :] >= 0)
        allowed_heads = jnp.broadcast_to(allowed[None, :, :], (HEADS, block_rows, SPAN * block_rows))
        result = lax.map(one_head, (jnp.transpose(query_block, (1, 0, 2)), jnp.transpose(key_window, (1, 0, 2)), jnp.transpose(value_window, (1, 0, 2)), allowed_heads))
        return jnp.transpose(result, (1, 0, 2))

    attended = lax.map(one_block, jnp.arange(N_SEQ, dtype=jnp.int32))
    attended = attended.reshape(TOKENS, HEADS * HEAD_DIM)
    coef_in = dwa_table[0][dwa_slot]
    coef_out = dwa_table[1][dwa_slot]
    layer_in = jnp.zeros((TOKENS, HEADS * HEAD_DIM), jnp.float32)
    extra = jnp.zeros((TOKENS, HEADS * HEAD_DIM), jnp.float32)
    for index in range(PAST):
        stored = past_outputs[index].astype(jnp.float32)
        layer_in = layer_in + coef_in[index] * stored
        extra = extra + coef_out[index] * stored
    hidden = layer_in + attended.astype(jnp.float32)
    return (hidden + extra).astype(jnp.bfloat16)
```

```python
import functools
import math

import jax
import jax.numpy as jnp
from jax import lax
from jax.experimental import pallas as pl
from jax.experimental.pallas import tpu as pltpu
from jax.sharding import PartitionSpec as P

HEAD_DIM = 128
SPAN = 4
STAT = 16
MESH = pl.DeviceIdType.MESH
Q, K, V = 0, 1, 2


def from_behind(block, axis, distance):
    devices = range(lax.axis_size(axis))
    route = [(i - distance, i) for i in devices if i - distance in devices]
    return lax.ppermute(block, axis, route)


def block_update(state, query_heads, key_heads, value_heads, allowed):
    running, total, accumulated = state
    scores = jnp.einsum("qhd,khd->hqk", query_heads, key_heads, preferred_element_type=jnp.float32)
    scores = scores * (1.0 / HEAD_DIM**0.5)
    scores = jnp.where(allowed, scores, -jnp.inf)
    new_max = jnp.maximum(running, jnp.max(scores, axis=2))
    factor = jnp.exp(running - new_max)
    prob = jnp.exp(scores - new_max[:, :, None])
    total = total * factor + jnp.sum(prob, axis=2)
    weights = prob.astype(jnp.bfloat16)
    update = jnp.einsum("hqk,khd->qhd", weights, value_heads, preferred_element_type=jnp.float32)
    accumulated = accumulated * jnp.transpose(factor)[:, :, None] + update
    return (new_max, total, accumulated)


def shards(queries, keys, values, past_outputs, dwa_slot, dwa_table):
    n_uly = lax.axis_size("uly")
    n_seq = lax.axis_size("seq")
    span_size = min(4, n_seq)
    features = queries.shape[1]
    local_heads = features // n_uly // HEAD_DIM
    query_rows, key_rows, value_rows = (
        lax.all_to_all(queries, "uly", split_axis=1, concat_axis=0, tiled=True),
        lax.all_to_all(keys, "uly", split_axis=1, concat_axis=0, tiled=True),
        lax.all_to_all(values, "uly", split_axis=1, concat_axis=0, tiled=True),
    )
    row_count = query_rows.shape[0]
    split_shape = (row_count, local_heads, HEAD_DIM)
    query_heads = query_rows.reshape(split_shape)
    table_index = jnp.arange(dwa_table.shape[1])
    onehot = (dwa_slot[:, None] == table_index[None, :]).astype(jnp.float32)
    coefs = jnp.dot(onehot, jnp.transpose(dwa_table), precision=lax.Precision.HIGHEST)
    layer_in = jnp.zeros(queries.shape, jnp.float32)
    extra = jnp.zeros(queries.shape, jnp.float32)
    for index in range(past_outputs.shape[0]):
        stored = past_outputs[index].astype(jnp.float32)
        layer_in = layer_in + coefs[index, 0] * stored
        extra = extra + coefs[index, 1] * stored
    running = jnp.full((local_heads, row_count), -jnp.inf, jnp.float32)
    total = jnp.zeros((local_heads, row_count), jnp.float32)
    accumulated = jnp.zeros(split_shape, jnp.float32)
    state = (running, total, accumulated)
    causal = (jnp.arange(row_count)[:, None] >= jnp.arange(row_count)[None, :])[None, :, :]
    state = block_update(
        state, query_heads, key_rows.reshape(split_shape), value_rows.reshape(split_shape), causal
    )
    position = lax.axis_index("seq")
    current = (key_rows, value_rows)
    for offset in range(1, span_size):
        current = from_behind((current[0], current[1]), "seq", 1)
        far_keys = current[0].reshape(split_shape)
        far_values = current[1].reshape(split_shape)

        def take_block(carry, far_keys=far_keys, far_values=far_values):
            return block_update(carry, query_heads, far_keys, far_values, True)

        def keep_block(carry):
            return carry

        state = lax.cond(position >= offset, take_block, keep_block, state)
    running, total, accumulated = state
    attended = accumulated / jnp.transpose(total)[:, :, None]
    attended = attended.astype(jnp.bfloat16).reshape(row_count, local_heads * HEAD_DIM)
    returned = lax.all_to_all(attended, "uly", split_axis=0, concat_axis=1, tiled=True)
    hidden = layer_in + returned.astype(jnp.float32)
    return (hidden + extra).astype(jnp.bfloat16)


def fused_kernel(
    shape,
    slot_ref, table_ref, q_hbm, k_hbm, v_hbm, past_hbm, back, base_ref,
    given, past, heads, own, own_stat, part_out, part_in, att,
    load_sem, past_sem, plane_sem, line_sem, heads_sem, part_send, part_recv, att_sem, back_sem,
):
    n_seq, n_uly, group = shape
    tokens = given.shape[1]
    rows = n_uly * tokens
    half = rows // 2
    scale = math.log2(math.e) / HEAD_DIM**0.5
    s, t = lax.axis_index("seq"), lax.axis_index("uly")
    alone = group - 1
    shared = group - 1
    guest = 0
    late, visit = group, group + 1

    loads = [
        pltpu.make_async_copy(src, given.at[i], load_sem.at[i]) for i, src in enumerate((q_hbm, k_hbm, v_hbm))
    ]
    for load in loads:
        load.start()
    past_load = pltpu.make_async_copy(past_hbm, past, past_sem)
    past_load.start()

    barrier = pltpu.get_barrier_semaphore()
    for d in range(1, n_uly):
        pl.semaphore_signal(barrier, inc=1, device_id={"uly": lax.rem(t + d, n_uly)}, device_id_type=MESH)
    for d in range(1, n_seq):
        pl.semaphore_signal(barrier, inc=1, device_id={"seq": lax.rem(s + d, n_seq)}, device_id_type=MESH)

    @pl.when(s == 3)
    def _():
        for d in range(1, n_uly):
            pl.semaphore_signal(
                barrier, inc=1, device_id={"seq": 2, "uly": lax.rem(t + d, n_uly)}, device_id_type=MESH
            )

    pl.semaphore_wait(barrier, n_uly + n_seq - 2 + jnp.where(s == 2, n_uly - 1, 0))
    for load in loads:
        load.wait()

    def columns(uly, g):
        return pl.ds(pl.multiple_of((uly * group + g) * HEAD_DIM, HEAD_DIM), HEAD_DIM)

    my_rows = pl.ds(pl.multiple_of(t * tokens, tokens), tokens)

    def plane(kind, g, d):
        peer = lax.rem(t + d, n_uly)
        src = given.at[kind, :, columns(peer, g)]
        dst = heads.at[kind, g, s, my_rows, :]
        if d == 0:
            return pltpu.make_async_copy(src, dst, heads_sem.at[kind, g, s])
        return pltpu.make_async_remote_copy(
            src, dst, plane_sem.at[kind, g, d], heads_sem.at[kind, g, s],
            device_id={"uly": peer}, device_id_type=MESH,
        )

    def scatter(kind, g):
        for d in (*range(1, n_uly), 0):
            plane(kind, g, d).start()

    def arrived(kind, g, block):
        ref = heads.at[kind, g, block]
        pltpu.make_async_copy(ref, ref, heads_sem.at[kind, g, block]).wait()

    def line(kind, g, to, lane=0, block=None):
        block = s if block is None else block
        ref = heads.at[kind, g, block]
        return pltpu.make_async_remote_copy(
            ref, ref, line_sem.at[kind, g, lane], heads_sem.at[kind, g, block],
            device_id={"seq": to}, device_id_type=MESH,
        )

    def partial(g, block, to=None, slot=None):
        slot = g if slot is None else slot
        return pltpu.make_async_remote_copy(
            part_out.at[g, block - n_seq // 2], part_in.at[slot],
            part_send.at[g, block - n_seq // 2], part_recv.at[slot],
            device_id={"seq": block if to is None else to}, device_id_type=MESH,
        )

    def returning(g, lane, block, d):
        peer = lax.rem(t + d, n_uly)
        src = att.at[lane, g, pl.ds(pl.multiple_of(peer * tokens, tokens), tokens), :]
        dst = back.at[:, columns(t, g)]
        if block is None and d == 0:
            return pltpu.make_async_copy(src, dst, back_sem.at[g, t])
        where = {"uly": peer} if block is None else {"seq": block, "uly": peer}
        return pltpu.make_async_remote_copy(
            src, dst, att_sem.at[lane, g, d], back_sem.at[g, t], device_id=where, device_id_type=MESH,
        )

    def give_back(g, lane=0, block=None):
        for d in (*range(1, n_uly), 0):
            returning(g, lane, block, d).start()

    def attend(g, block, full, diagonal, finish, resume=None):
        for a in range(2):
            query = heads[Q, g, block, a * half:(a + 1) * half, :]
            top = total = acc = None
            if resume is not None:
                cut = slice(a * half, (a + 1) * half)
                top, total, acc = own_stat[resume, 0:1, cut], own_stat[resume, 1:2, cut], own[resume, :, cut]
            spans = [(j, rows, False) for j in full] + ([(block, (a + 1) * half, True)] if diagonal else [])
            for j, count, masked in spans:
                key = heads[K, g, j, 0:count, :]
                value = heads[V, g, j, 0:count, :]
                scores = lax.dot_general(key, query, (((1,), (1,)), ((), ())), preferred_element_type=jnp.float32)
                scores = scores * scale
                if masked:
                    key_at = lax.broadcasted_iota(jnp.int32, scores.shape, 0)
                    query_at = lax.broadcasted_iota(jnp.int32, scores.shape, 1) + a * half
                    scores = jnp.where(key_at <= query_at, scores, -jnp.inf)
                peak = jnp.max(scores, axis=0, keepdims=True)
                new_top = peak if top is None else jnp.maximum(top, peak)
                prob = jnp.exp2(scores - new_top)
                sums = jnp.sum(prob, axis=0, keepdims=True)
                update = lax.dot_general(
                    value, prob.astype(jnp.bfloat16), (((0,), (0,)), ((), ())), preferred_element_type=jnp.float32
                )
                if top is None:
                    total, acc = sums, update
                else:
                    factor = jnp.exp2(top - new_top)
                    total = total * factor + sums
                    acc = acc * factor + update
                top = new_top
            finish(slice(a * half, (a + 1) * half), top, total, acc)

    def settle(g, lane=0):
        def finish(cut, top, total, acc):
            att[lane, g, cut, :] = jnp.transpose(acc / total).astype(jnp.bfloat16)
        return finish

    def keep(g):
        def finish(cut, top, total, acc):
            own[g, :, cut] = acc
            own_stat[g, 0:1, cut] = top
            own_stat[g, 1:2, cut] = total
        return finish

    def hand_over(g, where):
        def finish(cut, top, total, acc):
            part_out[g, where, 0:HEAD_DIM, cut] = (acc / total).astype(jnp.bfloat16)
            level = top + jnp.log2(total)
            high = level.astype(jnp.bfloat16).astype(jnp.float32)
            middle = (level - high).astype(jnp.bfloat16).astype(jnp.float32)
            low = level - high - middle
            row = lax.broadcasted_iota(jnp.int32, (STAT, half), 0)
            stats = jnp.where(row == 0, high, jnp.where(row == 1, middle, jnp.where(row == 2, low, 0.0)))
            part_out[g, where, HEAD_DIM:HEAD_DIM + STAT, cut] = stats.astype(jnp.bfloat16)
        return finish

    def merge(g, slot=None, lane=0):
        slot = g if slot is None else slot
        pltpu.make_async_copy(part_in.at[slot], part_in.at[slot], part_recv.at[slot]).wait()
        for a in range(2):
            cut = slice(a * half, (a + 1) * half)
            stats = part_in[slot, HEAD_DIM:HEAD_DIM + STAT, cut].astype(jnp.float32)
            level = stats[0:1] + stats[1:2] + stats[2:3]
            top, total = own_stat[slot, 0:1, cut], own_stat[slot, 1:2, cut]
            new_top = jnp.maximum(top, level)
            mine, theirs = jnp.exp2(top - new_top), jnp.exp2(level - new_top)
            inverse = 1.0 / (total * mine + theirs)
            other = part_in[slot, 0:HEAD_DIM, cut].astype(jnp.float32)
            both = own[slot, :, cut] * (mine * inverse) + other * (theirs * inverse)
            att[lane, g, cut, :] = jnp.transpose(both).astype(jnp.bfloat16)

    def each(first, count, body):
        def step(g, carry):
            body(g)
            return carry
        lax.fori_loop(first, count, step, 0)

    upward = (*range(shared - 1), alone, shared - 1)

    @pl.when(s == 0)
    def _():
        for g in upward:
            scatter(K, g)
            scatter(V, g)
        for g in upward:
            scatter(Q, g)
        for g in upward:
            for kind in (K, V):
                arrived(kind, g, 0)
                line(kind, g, 1).start()

        def work(g):
            arrived(Q, g, 0)
            attend(g, 0, (), True, settle(g))
            give_back(g)
        each(0, group, work)

    @pl.when(s == 1)
    def _():
        scatter(K, alone)
        scatter(V, alone)
        for g in range(shared):
            scatter(K, g)
            scatter(V, g)
        for g in range(group):
            scatter(Q, g)
        for kind in (K, V):
            arrived(kind, alone, 1)
            line(kind, alone, 2).start()

        def far(g, last=3, slot=None):
            for kind in (K, V):
                arrived(kind, g, 1)
                arrived(kind, g, 0)
            for block in (2, 3):
                arrived(Q, g, block)
                attend(g, block, (0, 1), False, hand_over(g, block - n_seq // 2))
                if block == 3:
                    partial(g, block, last, slot).start()
                else:
                    partial(g, block).start()
        def near(g):
            arrived(Q, g, 1)
            attend(g, 1, (0,), True, settle(g))
            give_back(g)
        if guest == shared - 1:
            for kind in (K, V):
                arrived(kind, alone, 0)
                line(kind, alone, 2, 1, 0).start()
        far(guest, 2, visit)
        each(1, shared - 1, far)
        each(0, shared - 1, near)
        if guest < shared - 1:
            for kind in (K, V):
                arrived(kind, alone, 0)
                line(kind, alone, 2, 1, 0).start()
        each(alone, group, near)
        if guest < shared - 1:
            far(shared - 1)
        each(shared - 1, shared, near)

    @pl.when(s == 2)
    def _():
        for g in range(shared):
            scatter(Q, g)
        for g in (*range(1, shared), guest):
            scatter(K, g)
            scatter(V, g)
        for kind in (Q, K, V):
            scatter(kind, alone)
        for g in range(shared):
            arrived(Q, g, 2)
            line(Q, g, 1).start()
            arrived(Q, g, 3)
            line(Q, g, 1, 1, 3).start()
            if g > 0:
                for kind in (K, V):
                    arrived(kind, g, 2)
                    line(kind, g, 3).start()
        for kind in (K, V):
            arrived(kind, guest, 2)

        def near(g):
            attend(g, 2, (), True, keep(g))
        each(0, shared, near)
        for kind in (K, V):
            arrived(kind, guest, 3)
        attend(guest, 3, (2,), True, keep(visit))

        def join(g):
            merge(g)
            give_back(g)
        join(guest)
        for kind in (K, V):
            arrived(kind, alone, 1)
        for kind in (Q, K, V):
            arrived(kind, alone, 2)
        attend(alone, 2, (1,), True, keep(alone))
        merge(guest, visit, 1)
        give_back(guest, 1, 3)
        for kind in (Q, K, V):
            arrived(kind, alone, 3)
        attend(alone, 3, (1, 2), True, keep(late))
        each(1, shared - 1, join)
        for kind in (K, V):
            arrived(kind, alone, 0)
        attend(alone, 3, (0,), False, settle(alone, 1), late)
        give_back(alone, 1, 3)
        attend(alone, 2, (0,), False, settle(alone), alone)
        give_back(alone)
        each(max(1, shared - 1), shared, join)

    @pl.when(s == 3)
    def _():
        for g in range(shared):
            scatter(Q, g)
        for kind in (K, V):
            scatter(kind, guest)
        for g in range(1, shared):
            scatter(K, g)
            scatter(V, g)
        for kind in (Q, K, V):
            scatter(kind, alone)
        for g in range(shared):
            arrived(Q, g, 3)
            line(Q, g, 2).start()
        for kind in (K, V):
            arrived(kind, guest, 3)
            line(kind, guest, 2).start()
        for kind in (Q, K, V):
            arrived(kind, alone, 3)
            line(kind, alone, 2).start()

        def near(g):
            for kind in (K, V):
                arrived(kind, g, 3)
                arrived(kind, g, 2)
            attend(g, 3, (2,), True, keep(g))
        each(1, shared, near)

        def join(g):
            merge(g)
            give_back(g)
        each(1, shared, join)

    past_load.wait()
    weights = [table_ref[0, slot_ref[p]] + table_ref[1, slot_ref[p]] for p in range(past.shape[0])]

    def combine(g):
        for uly in range(n_uly):
            cols = columns(uly, g)
            mixed = weights[0] * past[0, :, cols].astype(jnp.float32)
            for p, weight in enumerate(weights[1:], 1):
                mixed = mixed + weight * past[p, :, cols].astype(jnp.float32)
            base_ref[:, cols] = mixed

    def landed(g):
        for uly in range(n_uly):
            cols = columns(uly, g)
            pltpu.make_async_copy(back.at[:, cols], back.at[:, cols], back_sem.at[g, uly]).wait()
    each(0, group, combine)
    each(0, group, landed)

    for g in range(group):
        for d in range(1, n_uly):
            for kind in (Q, K, V):
                plane(kind, g, d).wait_send()

    def returned(g, lane=0, block=None):
        for d in range(0 if block is not None else 1, n_uly):
            returning(g, lane, block, d).wait_send()

    @pl.when(s == 0)
    def _():
        for g in range(group):
            for kind in (K, V):
                line(kind, g, 1).wait_send()
            returned(g)

    @pl.when(s == 1)
    def _():
        for kind in (K, V):
            line(kind, alone, 2).wait_send()
            line(kind, alone, 2, 1, 0).wait_send()
        for g in range(shared):
            for block in (2, 3):
                partial(g, block).wait_send()
        for g in range(group):
            returned(g)

    @pl.when(s == 2)
    def _():
        for g in range(shared):
            line(Q, g, 1).wait_send()
            line(Q, g, 1, 1, 3).wait_send()
        for g in range(1, shared):
            for kind in (K, V):
                line(kind, g, 3).wait_send()
        for g in range(group):
            returned(g)
        for g in (guest, alone):
            returned(g, 1, 3)

    @pl.when(s == 3)
    def _():
        for g in range(shared):
            line(Q, g, 2).wait_send()
        for kind in (K, V):
            line(kind, guest, 2).wait_send()
        for g in range(1, shared):
            returned(g)
        for kind in (Q, K, V):
            line(kind, alone, 2).wait_send()


def fused(queries, keys, values, past_outputs, dwa_slot, dwa_table):
    n_seq, n_uly = lax.axis_size("seq"), lax.axis_size("uly")
    tokens, features = queries.shape
    group = features // n_uly // HEAD_DIM
    rows = tokens * n_uly
    stored = past_outputs.shape[0]
    bf16, f32 = jnp.bfloat16, jnp.float32
    anywhere = pl.BlockSpec(memory_space=pltpu.HBM)
    scalars = pl.BlockSpec(memory_space=pltpu.SMEM)
    attended, base = pl.pallas_call(
        functools.partial(fused_kernel, (n_seq, n_uly, group)),
        out_shape=(pltpu.VMEM((tokens, features), bf16), pltpu.VMEM((tokens, features), f32)),
        in_specs=[scalars, scalars, anywhere, anywhere, anywhere, anywhere],
        out_specs=[pl.BlockSpec(memory_space=pltpu.VMEM)] * 2,
        scratch_shapes=[
            pltpu.VMEM((3, tokens, features), bf16),
            pltpu.VMEM((stored, tokens, features), bf16),
            pltpu.VMEM((3, group, n_seq, rows, HEAD_DIM), bf16),
            pltpu.VMEM((group + 2, HEAD_DIM, rows), f32),
            pltpu.VMEM((group + 2, 8, rows), f32),
            pltpu.VMEM((group, 2, HEAD_DIM + STAT, rows), bf16),
            pltpu.VMEM((group + 2, HEAD_DIM + STAT, rows), bf16),
            pltpu.VMEM((2, group, rows, HEAD_DIM), bf16),
            pltpu.SemaphoreType.DMA((3,)),
            pltpu.SemaphoreType.DMA,
            pltpu.SemaphoreType.DMA((3, group, n_uly)),
            pltpu.SemaphoreType.DMA((3, group, 2)),
            pltpu.SemaphoreType.DMA((3, group, n_seq)),
            pltpu.SemaphoreType.DMA((group, 2)),
            pltpu.SemaphoreType.DMA((group + 2,)),
            pltpu.SemaphoreType.DMA((2, group, n_uly)),
            pltpu.SemaphoreType.DMA((group, n_uly)),
        ],
        compiler_params=pltpu.CompilerParams(
            collective_id=0, has_side_effects=True, vmem_limit_bytes=32 * 1024 * 1024
        ),
    )(*(pltpu.with_memory_space_constraint(x, pltpu.HBM) for x in (dwa_slot, dwa_table, queries, keys, values, past_outputs)))
    return (base + attended.astype(f32)).astype(bf16)


def solution(mesh):
    def body(queries, *rest):
        heads_here = queries.shape[1] // HEAD_DIM // mesh.shape["uly"]
        fits = mesh.shape["seq"] == SPAN and heads_here >= 2
        return (fused if fits else shards)(queries, *rest)

    return jax.shard_map(
        body,
        mesh=mesh,
        in_specs=(
            P(("rep", "seq", "uly"), None),
            P(("rep", "seq", "uly"), None),
            P(("rep", "seq", "uly"), None),
            P(None, ("rep", "seq", "uly"), None),
            P(),
            P(),
        ),
        out_specs=P(("rep", "seq", "uly"), None),
        check_vma=False,
    )
```

```python
import functools
import math

import jax
import jax.numpy as jnp
from jax import lax
from jax.experimental import pallas as pl
from jax.experimental.pallas import tpu as pltpu
from jax.sharding import PartitionSpec as P

HEAD_DIM = 128
SPAN = 4
PLANE = 4
STAT = 8
MESH = pl.DeviceIdType.MESH
Q, K, V = 0, 1, 2


def from_behind(block, axis, distance):
    devices = range(lax.axis_size(axis))
    route = [(i - distance, i) for i in devices if i - distance in devices]
    return lax.ppermute(block, axis, route)


def block_update(state, query_heads, key_heads, value_heads, allowed):
    running, total, accumulated = state
    scores = jnp.einsum("qhd,khd->hqk", query_heads, key_heads, preferred_element_type=jnp.float32)
    scores = scores * (1.0 / HEAD_DIM**0.5)
    scores = jnp.where(allowed, scores, -jnp.inf)
    new_max = jnp.maximum(running, jnp.max(scores, axis=2))
    factor = jnp.exp(running - new_max)
    prob = jnp.exp(scores - new_max[:, :, None])
    total = total * factor + jnp.sum(prob, axis=2)
    weights = prob.astype(jnp.bfloat16)
    update = jnp.einsum("hqk,khd->qhd", weights, value_heads, preferred_element_type=jnp.float32)
    accumulated = accumulated * jnp.transpose(factor)[:, :, None] + update
    return (new_max, total, accumulated)


def shards(queries, keys, values, past_outputs, dwa_slot, dwa_table):
    n_uly = lax.axis_size("uly")
    n_seq = lax.axis_size("seq")
    span_size = min(4, n_seq)
    features = queries.shape[1]
    local_heads = features // n_uly // HEAD_DIM
    query_rows, key_rows, value_rows = (
        lax.all_to_all(queries, "uly", split_axis=1, concat_axis=0, tiled=True),
        lax.all_to_all(keys, "uly", split_axis=1, concat_axis=0, tiled=True),
        lax.all_to_all(values, "uly", split_axis=1, concat_axis=0, tiled=True),
    )
    row_count = query_rows.shape[0]
    split_shape = (row_count, local_heads, HEAD_DIM)
    query_heads = query_rows.reshape(split_shape)
    table_index = jnp.arange(dwa_table.shape[1])
    onehot = (dwa_slot[:, None] == table_index[None, :]).astype(jnp.float32)
    coefs = jnp.dot(onehot, jnp.transpose(dwa_table), precision=lax.Precision.HIGHEST)
    layer_in = jnp.zeros(queries.shape, jnp.float32)
    extra = jnp.zeros(queries.shape, jnp.float32)
    for index in range(past_outputs.shape[0]):
        stored = past_outputs[index].astype(jnp.float32)
        layer_in = layer_in + coefs[index, 0] * stored
        extra = extra + coefs[index, 1] * stored
    running = jnp.full((local_heads, row_count), -jnp.inf, jnp.float32)
    total = jnp.zeros((local_heads, row_count), jnp.float32)
    accumulated = jnp.zeros(split_shape, jnp.float32)
    state = (running, total, accumulated)
    causal = (jnp.arange(row_count)[:, None] >= jnp.arange(row_count)[None, :])[None, :, :]
    state = block_update(
        state, query_heads, key_rows.reshape(split_shape), value_rows.reshape(split_shape), causal
    )
    position = lax.axis_index("seq")
    current = (key_rows, value_rows)
    for offset in range(1, span_size):
        current = from_behind((current[0], current[1]), "seq", 1)
        far_keys = current[0].reshape(split_shape)
        far_values = current[1].reshape(split_shape)

        def take_block(carry, far_keys=far_keys, far_values=far_values):
            return block_update(carry, query_heads, far_keys, far_values, True)

        def keep_block(carry):
            return carry

        state = lax.cond(position >= offset, take_block, keep_block, state)
    running, total, accumulated = state
    attended = accumulated / jnp.transpose(total)[:, :, None]
    attended = attended.astype(jnp.bfloat16).reshape(row_count, local_heads * HEAD_DIM)
    returned = lax.all_to_all(attended, "uly", split_axis=0, concat_axis=1, tiled=True)
    hidden = layer_in + returned.astype(jnp.float32)
    return (hidden + extra).astype(jnp.bfloat16)


def fused_kernel(
    shape,
    slot_ref, table_ref, q_hbm, k_hbm, v_hbm, past_hbm, back, base_ref,
    given, past, heads, own, own_stat, part_out, part_in, att,
    load_sem, past_sem, plane_send, piece_sem, whole_sem, line_send, guest_send, line_recv,
    relay_sem, part_send, part_recv, att_send, back_sem,
):
    n_seq, n_uly, group = shape
    tokens = given.shape[1]
    rows = n_uly * tokens
    half = rows // 2
    scale = math.log2(math.e) / HEAD_DIM**0.5
    s, t = lax.axis_index("seq"), lax.axis_index("uly")
    y, x = t // 2, t % 2
    peers = (t, 2 * y + 1 - x, 2 * (1 - y) + x, 3 - t)
    guests = range(max(1, group // 2))
    hosts = range(len(guests), group)
    visit = group

    loads = [
        pltpu.make_async_copy(src, given.at[i], load_sem.at[i]) for i, src in enumerate((q_hbm, k_hbm, v_hbm))
    ]
    past_load = pltpu.make_async_copy(past_hbm, past, past_sem)
    for load in loads:
        load.start()
    past_load.start()

    barrier = pltpu.get_barrier_semaphore()
    for d in (1, 2, 3):
        pl.semaphore_signal(barrier, inc=1, device_id={"uly": peers[d]}, device_id_type=MESH)
    neighbours = {0: (1,), 1: (0, 2, 3), 2: (1, 3), 3: (1, 2)}
    for place, others in neighbours.items():
        @pl.when(s == place)
        def _(place=place, others=others):
            for other in others:
                pl.semaphore_signal(barrier, inc=1, device_id={"seq": other}, device_id_type=MESH)
            if place == 3:
                for d in (1, 2, 3):
                    pl.semaphore_signal(barrier, inc=1, device_id={"seq": 2, "uly": peers[d]}, device_id_type=MESH)
            pl.semaphore_wait(barrier, 3 + len(others) + (3 if place == 2 else 0))
    for load in loads:
        load.wait()

    def columns(uly, g):
        return pl.ds(pl.multiple_of((uly * group + g) * HEAD_DIM, HEAD_DIM), HEAD_DIM)

    def row_range(uly):
        return pl.ds(pl.multiple_of(uly * tokens, tokens), tokens)

    def scatter(kind, g, pieces):
        for d in (1, 2, 3, 0):
            src = given.at[kind, :, columns(peers[d], g)]
            dst = heads.at[kind, g, s, row_range(t), :]
            sem = piece_sem.at[kind, g, d] if pieces else whole_sem.at[kind, g]
            if d == 0:
                pltpu.make_async_copy(src, dst, sem).start()
            else:
                pltpu.make_async_remote_copy(
                    src, dst, plane_send.at[kind], sem, device_id={"uly": peers[d]}, device_id_type=MESH
                ).start()

    def landed(ref, sem):
        pltpu.make_async_copy(ref, ref, sem).wait()

    def gathered(kind, g):
        landed(heads.at[kind, g, s], whole_sem.at[kind, g])

    def gathered_piece(kind, g, d):
        landed(heads.at[kind, g, s, row_range(peers[d]), :], piece_sem.at[kind, g, d])

    def arrived(kind, g, block):
        landed(heads.at[kind, g, block], line_recv.at[kind, g, block])

    def pass_on(kind, g, d, to, guest=False):
        dst = heads.at[kind, g, s, row_range(peers[d]), :]
        src = given.at[kind, :, columns(t, g)] if d == 0 else dst
        sem = relay_sem.at[g, d] if to == 2 and kind == Q and g > 0 else line_recv.at[kind, g, s]
        pltpu.make_async_remote_copy(
            src, dst, guest_send if guest else line_send.at[kind], sem, device_id={"seq": to}, device_id_type=MESH
        ).start()

    def relay(g, d):
        ref = heads.at[Q, g, 3, row_range(peers[d]), :]
        landed(ref, relay_sem.at[g, d])
        pltpu.make_async_remote_copy(
            ref, ref, guest_send, line_recv.at[Q, g, 3], device_id={"seq": 1}, device_id_type=MESH
        ).start()

    def partial(g, where, a, to, slot):
        pltpu.make_async_remote_copy(
            part_out.at[g, where, a], part_in.at[slot, a], part_send, part_recv.at[slot, a],
            device_id={"seq": to}, device_id_type=MESH,
        ).start()

    def give_back(g, ds, lane=0):
        for d in ds:
            src = att.at[lane, g, row_range(peers[d]), :]
            dst = back.at[:, columns(t, g)]
            if lane == 0 and d == 0:
                pltpu.make_async_copy(src, dst, back_sem).start()
                continue
            where = {"uly": peers[d]} if lane == 0 else {"seq": n_seq - 1, "uly": peers[d]}
            pltpu.make_async_remote_copy(
                src, dst, att_send.at[lane], back_sem, device_id=where, device_id_type=MESH
            ).start()

    def attend_half(g, block, a, full, diagonal, finish, resume=None):
        query = heads[Q, g, block, pl.ds(pl.multiple_of(a * half, half), half), :]
        top = total = acc = None
        if resume is not None:
            top, total, acc = own_stat[resume, a, 0:1, :], own_stat[resume, a, 1:2, :], own[resume, a]
        spans = [(j, rows, False) for j in full] + ([(block, (a + 1) * half, True)] if diagonal else [])
        for j, count, masked in spans:
            key = heads[K, g, j, 0:count, :]
            value = heads[V, g, j, 0:count, :]
            scores = lax.dot_general(key, query, (((1,), (1,)), ((), ())), preferred_element_type=jnp.float32)
            scores = scores * scale
            if masked:
                key_at = lax.broadcasted_iota(jnp.int32, scores.shape, 0)
                query_at = lax.broadcasted_iota(jnp.int32, scores.shape, 1) + a * half
                scores = jnp.where(key_at <= query_at, scores, -jnp.inf)
            peak = jnp.max(scores, axis=0, keepdims=True)
            new_top = peak if top is None else jnp.maximum(top, peak)
            prob = jnp.exp2(scores - new_top)
            sums = jnp.sum(prob, axis=0, keepdims=True)
            update = lax.dot_general(
                value, prob.astype(jnp.bfloat16), (((0,), (0,)), ((), ())), preferred_element_type=jnp.float32
            )
            if top is None:
                total, acc = sums, update
            else:
                factor = jnp.exp2(top - new_top)
                total = total * factor + sums
                acc = acc * factor + update
            top = new_top
        finish(a, top, total, acc)

    def attend(g, block, full, diagonal, finish, resume=None):
        for a in range(2):
            attend_half(g, block, a, full, diagonal, finish, resume)

    def att_rows(a):
        return pl.ds(pl.multiple_of(a * half, half), half)

    def settle(g):
        def finish(a, top, total, acc):
            att[0, g, att_rows(a), :] = jnp.transpose(acc / total).astype(jnp.bfloat16)
        return finish

    def keep(slot):
        def finish(a, top, total, acc):
            own[slot, a] = acc
            own_stat[slot, a, 0:1, :] = top
            own_stat[slot, a, 1:2, :] = total
        return finish

    def hand_over(g, where):
        def finish(a, top, total, acc):
            part_out[g, where, a, 0:HEAD_DIM, :] = (acc / total).astype(jnp.bfloat16)
            level = top + jnp.log2(total)
            high = level.astype(jnp.bfloat16).astype(jnp.float32)
            middle = (level - high).astype(jnp.bfloat16).astype(jnp.float32)
            low = level - high - middle
            row = lax.broadcasted_iota(jnp.int32, (STAT, half), 0)
            stats = jnp.where(row == 0, high, jnp.where(row == 1, middle, jnp.where(row == 2, low, 0.0)))
            part_out[g, where, a, HEAD_DIM:HEAD_DIM + STAT, :] = stats.astype(jnp.bfloat16)
        return finish

    def merge(g, slot, a, lane=0):
        landed(part_in.at[slot, a], part_recv.at[slot, a])
        stats = part_in[slot, a, HEAD_DIM:HEAD_DIM + STAT, :].astype(jnp.float32)
        level = stats[0:1] + stats[1:2] + stats[2:3]
        top, total = own_stat[slot, a, 0:1, :], own_stat[slot, a, 1:2, :]
        new_top = jnp.maximum(top, level)
        mine, theirs = jnp.exp2(top - new_top), jnp.exp2(level - new_top)
        inverse = 1.0 / (total * mine + theirs)
        other = part_in[slot, a, 0:HEAD_DIM, :].astype(jnp.float32)
        both = own[slot, a] * (mine * inverse) + other * (theirs * inverse)
        att[lane, g, att_rows(a), :] = jnp.transpose(both).astype(jnp.bfloat16)

    def join(g, slot=None, lane=0):
        slot = g if slot is None else slot
        merge(g, slot, 1 - y, lane)
        give_back(g, (3, 2), lane)
        merge(g, slot, y, lane)
        give_back(g, (1, 0), lane)

    def each(first, count, body):
        def step(g, carry):
            body(g)
            return carry
        lax.fori_loop(first, count, step, 0)

    def add_up():
        past_load.wait()
        weights = [table_ref[0, slot_ref[p]] + table_ref[1, slot_ref[p]] for p in range(past.shape[0])]

        def sum_columns(uly):
            cols = pl.ds(pl.multiple_of(uly * (group * HEAD_DIM), HEAD_DIM), group * HEAD_DIM)
            mixed = weights[0] * past[0, :, cols].astype(jnp.float32)
            for p in range(1, past.shape[0]):
                mixed = mixed + weights[p] * past[p, :, cols].astype(jnp.float32)
            base_ref[:, cols] = mixed
        each(0, n_uly, sum_columns)

    def plane_sent():
        for kind in (Q, K, V):
            ref = given.at[kind, :, 0:(n_uly - 1) * group * HEAD_DIM]
            landed(ref, plane_send.at[kind])

    def line_sent(kind, first=0):
        landed(heads.at[kind, first:, s], line_send.at[kind])

    def att_sent(first=0):
        landed(att.at[0, first:, 0:(n_uly - 1) * tokens, :], att_send.at[0])

    @pl.when(s == 0)
    def _():
        for kind in (K, V):
            pass_on(kind, 0, 0, 1)
        for g in range(group):
            scatter(K, g, True)
            scatter(V, g, True)
        for g in range(group):
            scatter(Q, g, False)
        order = [(kind, g) for g in range(group) for kind in (K, V)]
        for i, (kind, g) in enumerate(order):
            if i + 2 < len(order):
                pass_on(*order[i + 2], 0, 1)
            for d in (1, 2, 3):
                gathered_piece(kind, g, d)
                pass_on(kind, g, d, 1)
        add_up()

        def work(g):
            gathered(Q, g)
            for kind in (K, V):
                gathered_piece(kind, g, 0)
            attend(g, 0, (), True, settle(g))
            give_back(g, (3, 2, 1, 0))
        each(0, group, work)
        plane_sent()
        for kind in (K, V):
            line_sent(kind)
        att_sent()

    @pl.when(s == 1)
    def _():
        for g in range(group):
            for kind in (K, V, Q):
                scatter(kind, g, False)
        add_up()

        def send(g, block, a):
            if block == 2:
                partial(g, 0, a, 2, g)
            else:
                stays = g < len(guests)
                partial(g, 1, a, jnp.where(stays, 2, 3), jnp.where(stays, visit + g, g))

        def far(g, block, full, resume=None):
            for a in (1 - y, y):
                attend_half(g, block, a, full, False, hand_over(g, block - 2), resume)
                send(g, block, a)

        def near(g):
            gathered(Q, g)
            attend(g, 1, (0,), True, settle(g))
            give_back(g, (3, 2, 1, 0))

        def both(g):
            for kind in (K, V):
                gathered(kind, g)
            for block in (3, 2):
                arrived(Q, g, block)
            for kind in (K, V):
                arrived(kind, g, 0)
            for block in (3, 2):
                far(g, block, (1, 0))

        for kind in (K, V):
            gathered(kind, 0)
        arrived(Q, 0, 2)
        attend(0, 2, (1,), False, keep(0))
        for kind in (K, V):
            arrived(kind, 0, 0)
        far(0, 2, (0,), 0)
        arrived(Q, 0, 3)
        far(0, 3, (1, 0))

        def work(g):
            near(g - 1)
            both(g)
        each(1, group, work)
        near(group - 1)
        plane_sent()
        landed(part_out, part_send)
        att_sent()

    @pl.when(s == 2)
    def _():
        pass_on(Q, 0, 0, 1)
        for kind in (K, V):
            pass_on(kind, hosts[0], 0, 3)
        order = [(Q, 0), (Q, 1)]
        for g in hosts:
            order += [(K, g), (V, g)] + ([(Q, g)] if g > 1 else [])
        order += [(Q, g) for g in range(2, hosts[0])]
        for kind, g in order:
            scatter(kind, g, True)
        for g in guests:
            for kind in (K, V):
                scatter(kind, g, False)
        for kind, g in order:
            to = 1 if kind == Q else 3
            if (g > 0 if kind == Q else g > hosts[0]):
                pass_on(kind, g, 0, to)
            for d in (1, 2, 3):
                gathered_piece(kind, g, d)
                pass_on(kind, g, d, to)
            if kind == Q and g > 0:
                for d in range(n_uly):
                    relay(g, d)
        add_up()

        def near(g):
            attend(g, 2, (), True, keep(g))

        def host(g):
            for kind in (Q, K, V):
                gathered_piece(kind, g, 0)
            near(g)

        def own_guest(g):
            for kind in (K, V):
                gathered(kind, g)
            gathered_piece(Q, g, 0)
            near(g)

        def receive(g):
            if g == 0:
                arrived(Q, g, 3)
            for kind in (K, V):
                arrived(kind, g, 3)
            attend(g, 3, (2,), True, keep(visit + g))

        each(hosts[0], group, host)
        each(0, len(guests), own_guest)
        receive(0)
        join(0)
        join(0, visit, 1)
        for g in guests[1:]:
            join(g)
            receive(g)
            join(g, visit + g, 1)
        each(hosts[0], group, join)
        plane_sent()
        line_sent(Q)
        for kind in (K, V):
            line_sent(kind, hosts[0])
        landed(heads.at[Q, 1:, 3], guest_send)
        landed(att.at[1, 0:len(guests)], att_send.at[1])
        att_sent()

    @pl.when(s == 3)
    def _():
        pass_on(Q, 0, 0, 1)
        pass_on(Q, 1, 0, 2)
        for g in range(group):
            scatter(Q, g, True)
        for g in guests:
            for kind in (K, V):
                scatter(kind, g, True)
        for g in hosts:
            for kind in (K, V):
                scatter(kind, g, False)
        for g in range(group):
            if g > 1:
                pass_on(Q, g, 0, 2)
            for d in (1, 2, 3):
                gathered_piece(Q, g, d)
                pass_on(Q, g, d, 2 if g > 0 else 1)
        for d in range(n_uly):
            pass_on(Q, 0, d, 2, True)
        for g in guests:
            for kind in (K, V):
                pass_on(kind, g, 0, 2)
                for d in (1, 2, 3):
                    gathered_piece(kind, g, d)
                    pass_on(kind, g, d, 2)
        for g in guests:
            for kind in (Q, K, V):
                gathered_piece(kind, g, 0)
        add_up()

        def near(g):
            gathered_piece(Q, g, 0)
            for kind in (K, V):
                gathered(kind, g)
                arrived(kind, g, 2)
            attend(g, 3, (2,), True, keep(g))
        each(hosts[0], group, near)
        each(hosts[0], group, join)
        plane_sent()
        line_sent(Q)
        for kind in (K, V):
            landed(heads.at[kind, 0:len(guests), s], line_send.at[kind])
        landed(heads.at[Q, 0, s], guest_send)
        att_sent(hosts[0])

    landed(back, back_sem)


def fused(queries, keys, values, past_outputs, dwa_slot, dwa_table):
    n_seq, n_uly = lax.axis_size("seq"), lax.axis_size("uly")
    tokens, features = queries.shape
    group = features // n_uly // HEAD_DIM
    rows = tokens * n_uly
    slots = group + max(1, group // 2)
    stored = past_outputs.shape[0]
    bf16, f32 = jnp.bfloat16, jnp.float32
    anywhere = pl.BlockSpec(memory_space=pltpu.HBM)
    scalars = pl.BlockSpec(memory_space=pltpu.SMEM)
    attended, base = pl.pallas_call(
        functools.partial(fused_kernel, (n_seq, n_uly, group)),
        out_shape=(pltpu.VMEM((tokens, features), bf16), pltpu.VMEM((tokens, features), f32)),
        in_specs=[scalars, scalars, anywhere, anywhere, anywhere, anywhere],
        out_specs=[pl.BlockSpec(memory_space=pltpu.VMEM)] * 2,
        scratch_shapes=[
            pltpu.VMEM((3, tokens, features), bf16),
            pltpu.VMEM((stored, tokens, features), bf16),
            pltpu.VMEM((3, group, n_seq, rows, HEAD_DIM), bf16),
            pltpu.VMEM((slots, 2, HEAD_DIM, rows // 2), f32),
            pltpu.VMEM((slots, 2, 8, rows // 2), f32),
            pltpu.VMEM((group, 2, 2, HEAD_DIM + STAT, rows // 2), bf16),
            pltpu.VMEM((slots, 2, HEAD_DIM + STAT, rows // 2), bf16),
            pltpu.VMEM((2, group, rows, HEAD_DIM), bf16),
            pltpu.SemaphoreType.DMA((3,)),
            pltpu.SemaphoreType.DMA,
            pltpu.SemaphoreType.DMA((3,)),
            pltpu.SemaphoreType.DMA((3, group, n_uly)),
            pltpu.SemaphoreType.DMA((3, group)),
            pltpu.SemaphoreType.DMA((3,)),
            pltpu.SemaphoreType.DMA,
            pltpu.SemaphoreType.DMA((3, group, n_seq)),
            pltpu.SemaphoreType.DMA((group, n_uly)),
            pltpu.SemaphoreType.DMA,
            pltpu.SemaphoreType.DMA((slots, 2)),
            pltpu.SemaphoreType.DMA((2,)),
            pltpu.SemaphoreType.DMA,
        ],
        compiler_params=pltpu.CompilerParams(
            collective_id=0, has_side_effects=True, vmem_limit_bytes=32 * 1024 * 1024
        ),
    )(*(pltpu.with_memory_space_constraint(x, pltpu.HBM) for x in (dwa_slot, dwa_table, queries, keys, values, past_outputs)))
    return (base + attended.astype(f32)).astype(bf16)


def solution(mesh):
    def body(queries, *rest):
        heads_here = queries.shape[1] // HEAD_DIM // mesh.shape["uly"]
        fits = mesh.shape["seq"] == SPAN and mesh.shape["uly"] == PLANE and heads_here >= 2
        return (fused if fits else shards)(queries, *rest)

    return jax.shard_map(
        body,
        mesh=mesh,
        in_specs=(
            P(("rep", "seq", "uly"), None),
            P(("rep", "seq", "uly"), None),
            P(("rep", "seq", "uly"), None),
            P(None, ("rep", "seq", "uly"), None),
            P(),
            P(),
        ),
        out_specs=P(("rep", "seq", "uly"), None),
        check_vma=False,
    )
```

```python
import functools
import math

import jax
import jax.numpy as jnp
from jax import lax
from jax.experimental import pallas as pl
from jax.experimental.pallas import tpu as pltpu
from jax.sharding import PartitionSpec as P

HEAD_DIM = 128
SPAN = 4
PLANE = 4
STAT = 8
MESH = pl.DeviceIdType.MESH
Q, K, V = 0, 1, 2


def from_behind(block, axis, distance):
    devices = range(lax.axis_size(axis))
    route = [(i - distance, i) for i in devices if i - distance in devices]
    return lax.ppermute(block, axis, route)


def block_update(state, query_heads, key_heads, value_heads, allowed):
    running, total, accumulated = state
    scores = jnp.einsum("qhd,khd->hqk", query_heads, key_heads, preferred_element_type=jnp.float32)
    scores = scores * (1.0 / HEAD_DIM**0.5)
    scores = jnp.where(allowed, scores, -jnp.inf)
    new_max = jnp.maximum(running, jnp.max(scores, axis=2))
    factor = jnp.exp(running - new_max)
    prob = jnp.exp(scores - new_max[:, :, None])
    total = total * factor + jnp.sum(prob, axis=2)
    weights = prob.astype(jnp.bfloat16)
    update = jnp.einsum("hqk,khd->qhd", weights, value_heads, preferred_element_type=jnp.float32)
    accumulated = accumulated * jnp.transpose(factor)[:, :, None] + update
    return (new_max, total, accumulated)


def shards(queries, keys, values, past_outputs, dwa_slot, dwa_table):
    n_uly = lax.axis_size("uly")
    n_seq = lax.axis_size("seq")
    span_size = min(4, n_seq)
    features = queries.shape[1]
    local_heads = features // n_uly // HEAD_DIM
    query_rows, key_rows, value_rows = (
        lax.all_to_all(queries, "uly", split_axis=1, concat_axis=0, tiled=True),
        lax.all_to_all(keys, "uly", split_axis=1, concat_axis=0, tiled=True),
        lax.all_to_all(values, "uly", split_axis=1, concat_axis=0, tiled=True),
    )
    row_count = query_rows.shape[0]
    split_shape = (row_count, local_heads, HEAD_DIM)
    query_heads = query_rows.reshape(split_shape)
    table_index = jnp.arange(dwa_table.shape[1])
    onehot = (dwa_slot[:, None] == table_index[None, :]).astype(jnp.float32)
    coefs = jnp.dot(onehot, jnp.transpose(dwa_table), precision=lax.Precision.HIGHEST)
    layer_in = jnp.zeros(queries.shape, jnp.float32)
    extra = jnp.zeros(queries.shape, jnp.float32)
    for index in range(past_outputs.shape[0]):
        stored = past_outputs[index].astype(jnp.float32)
        layer_in = layer_in + coefs[index, 0] * stored
        extra = extra + coefs[index, 1] * stored
    running = jnp.full((local_heads, row_count), -jnp.inf, jnp.float32)
    total = jnp.zeros((local_heads, row_count), jnp.float32)
    accumulated = jnp.zeros(split_shape, jnp.float32)
    state = (running, total, accumulated)
    causal = (jnp.arange(row_count)[:, None] >= jnp.arange(row_count)[None, :])[None, :, :]
    state = block_update(
        state, query_heads, key_rows.reshape(split_shape), value_rows.reshape(split_shape), causal
    )
    position = lax.axis_index("seq")
    current = (key_rows, value_rows)
    for offset in range(1, span_size):
        current = from_behind((current[0], current[1]), "seq", 1)
        far_keys = current[0].reshape(split_shape)
        far_values = current[1].reshape(split_shape)

        def take_block(carry, far_keys=far_keys, far_values=far_values):
            return block_update(carry, query_heads, far_keys, far_values, True)

        def keep_block(carry):
            return carry

        state = lax.cond(position >= offset, take_block, keep_block, state)
    running, total, accumulated = state
    attended = accumulated / jnp.transpose(total)[:, :, None]
    attended = attended.astype(jnp.bfloat16).reshape(row_count, local_heads * HEAD_DIM)
    returned = lax.all_to_all(attended, "uly", split_axis=0, concat_axis=1, tiled=True)
    hidden = layer_in + returned.astype(jnp.float32)
    return (hidden + extra).astype(jnp.bfloat16)


def fused_kernel(
    shape,
    slot_ref, table_ref, q_hbm, k_hbm, v_hbm, past_hbm, back, base_ref,
    given, past, heads, own, own_stat, part_out, part_in, att, last_out, last_in,
    load_sem, past_sem, plane_send, piece_sem, relay_sem, whole_sem, line_send, extra_send, line_recv,
    part_send, part_recv, att_send, back_sem, last_send, last_own, last_far,
):
    n_seq, n_uly, group = shape
    tokens = given.shape[1]
    rows = n_uly * tokens
    half = rows // 2
    scale = math.log2(math.e) / HEAD_DIM**0.5
    s, t = lax.axis_index("seq"), lax.axis_index("uly")
    y, x = t // 2, t % 2
    peers = (t, 2 * y + 1 - x, 2 * (1 - y) + x, 3 - t)
    guests = range(max(1, group // 2))
    hosts = range(len(guests), group)
    visit = group
    lanes = {(Q, 2): 0, (Q, 3): 1, (K, 0): 2, (V, 0): 3, (K, 2): 2, (V, 2): 3, (K, 3): 2, (V, 3): 3}

    loads = [
        pltpu.make_async_copy(src, given.at[i], load_sem) for i, src in enumerate((q_hbm, k_hbm, v_hbm))
    ]
    past_load = pltpu.make_async_copy(past_hbm, past, past_sem)
    for load in loads:
        load.start()
    past_load.start()

    def landed(ref, sem):
        pltpu.make_async_copy(ref, ref, sem).wait()

    barrier = pltpu.get_barrier_semaphore()
    for d in (1, 2, 3):
        pl.semaphore_signal(barrier, inc=1, device_id={"uly": peers[d]}, device_id_type=MESH)
    neighbours = {0: (1,), 1: (0, 2, 3), 2: (1, 3), 3: (1, 2)}
    for place, others in neighbours.items():
        @pl.when(s == place)
        def _(place=place, others=others):
            for other in others:
                pl.semaphore_signal(barrier, inc=1, device_id={"seq": other}, device_id_type=MESH)
            if place == 3:
                for d in (1, 2, 3):
                    pl.semaphore_signal(barrier, inc=1, device_id={"seq": 2, "uly": peers[d]}, device_id_type=MESH)
            pl.semaphore_wait(barrier, 3 + len(others) + (3 if place == 2 else 0))
    landed(given, load_sem)

    def columns(uly, g):
        return pl.ds(pl.multiple_of((uly * group + g) * HEAD_DIM, HEAD_DIM), HEAD_DIM)

    def row_range(uly):
        return pl.ds(pl.multiple_of(uly * tokens, tokens), tokens)

    def scatter(kind, g, pieces=None):
        for d in (1, 2, 3, 0):
            src = given.at[kind, :, columns(peers[d], g)]
            dst = heads.at[kind, g, s, row_range(t), :]
            sem = whole_sem.at[kind, g] if pieces is None else piece_sem.at[pieces, d]
            if d == 0:
                pltpu.make_async_copy(src, dst, sem).start()
            else:
                pltpu.make_async_remote_copy(
                    src, dst, plane_send, sem, device_id={"uly": peers[d]}, device_id_type=MESH
                ).start()

    def gathered(kind, g):
        landed(heads.at[kind, g, s], whole_sem.at[kind, g])

    def gathered_piece(kind, g, d, pieces):
        landed(heads.at[kind, g, s, row_range(peers[d]), :], piece_sem.at[pieces, d])

    def arrived(kind, g, block):
        landed(heads.at[kind, g, block], line_recv.at[lanes[kind, block], g])

    def pass_on(kind, g, d, block, to, send=None):
        dst = heads.at[kind, g, block, row_range(peers[d]), :]
        src = given.at[kind, :, columns(t, g)] if d == 0 else dst
        piecewise = kind == Q and block == 3 and to == 2 and g == 1
        sem = relay_sem.at[d] if piecewise else line_recv.at[lanes[kind, block], g]
        pltpu.make_async_remote_copy(
            src, dst, line_send.at[kind] if send is None else send, sem,
            device_id={"seq": to}, device_id_type=MESH,
        ).start()

    def forward(kind, g, block, to, pieces=None):
        if pieces is None:
            gathered(kind, g)
        for d in (1, 2, 3):
            if pieces is not None:
                gathered_piece(kind, g, d, pieces)
            pass_on(kind, g, d, block, to)

    def relay(g):
        parts = [heads.at[Q, g, 3]]
        if g == 1:
            parts = [heads.at[Q, g, 3, row_range(peers[d]), :] for d in range(n_uly)]
        for d, ref in enumerate(parts):
            landed(ref, relay_sem.at[d] if g == 1 else line_recv.at[lanes[Q, 3], g])
            pltpu.make_async_remote_copy(
                ref, ref, extra_send, line_recv.at[lanes[Q, 3], g], device_id={"seq": 1}, device_id_type=MESH
            ).start()

    def partial(g, where, a, to, slot):
        pltpu.make_async_remote_copy(
            part_out.at[g, where, a], part_in.at[slot, a], part_send, part_recv.at[slot, a],
            device_id={"seq": to}, device_id_type=MESH,
        ).start()

    def give_back(g, ds, lane=0):
        for d in ds:
            src = att.at[lane, g, row_range(peers[d]), :]
            dst = back.at[:, columns(t, g)]
            if lane == 0 and d == 0:
                pltpu.make_async_copy(src, dst, back_sem).start()
                continue
            where = {"uly": peers[d]} if lane == 0 else {"seq": n_seq - 1, "uly": peers[d]}
            pltpu.make_async_remote_copy(
                src, dst, att_send.at[lane], back_sem, device_id=where, device_id_type=MESH
            ).start()

    def attend(g, block, full, diagonal, finish, resume=None):
        query = heads[Q, g, block]
        acc_shape = (rows, HEAD_DIM)
        top = total = acc = None
        if resume is not None:
            top, total, acc = own_stat[resume, 0], own_stat[resume, 1], own[resume]
        for j in (*full, block) if diagonal else full:
            key = heads[K, g, j]
            value = heads[V, g, j]
            scores = lax.dot_general(query, key, (((1,), (1,)), ((), ())), preferred_element_type=jnp.float32)
            scores = scores * scale
            if j == block:
                query_at = lax.broadcasted_iota(jnp.int32, scores.shape, 0)
                key_at = lax.broadcasted_iota(jnp.int32, scores.shape, 1)
                scores = jnp.where(key_at <= query_at, scores, -jnp.inf)
            peak = jnp.broadcast_to(jnp.max(scores, axis=1, keepdims=True), acc_shape)
            new_top = peak if top is None else jnp.maximum(top, peak)
            prob = jnp.exp2(scores - jnp.concatenate([new_top] * (rows // HEAD_DIM), axis=1))
            sums = jnp.broadcast_to(jnp.sum(prob, axis=1, keepdims=True), acc_shape)
            update = jnp.dot(prob.astype(jnp.bfloat16), value, preferred_element_type=jnp.float32)
            if top is None:
                total, acc = sums, update
            else:
                factor = jnp.exp2(top - new_top)
                total = total * factor + sums
                acc = acc * factor + update
            top = new_top
        finish(top, total, acc)

    def settle(g):
        def finish(top, total, acc):
            att[0, g] = (acc / total).astype(jnp.bfloat16)
        return finish

    def keep(slot):
        def finish(top, total, acc):
            own[slot] = acc
            own_stat[slot, 0] = top
            own_stat[slot, 1] = total
        return finish

    def selector(shape, dim, chunk):
        place = lax.broadcasted_iota(jnp.int32, shape, dim) - 3 * chunk
        other = lax.broadcasted_iota(jnp.int32, shape, 1 - dim)
        return place, other

    def packed(top, total):
        level = top + jnp.log2(total)
        high = level.astype(jnp.bfloat16).astype(jnp.float32)
        middle = (level - high).astype(jnp.bfloat16).astype(jnp.float32)
        low = level - high - middle
        lane = lax.broadcasted_iota(jnp.int32, (rows, HEAD_DIM), 1)
        split = jnp.where(lane == 0, high, jnp.where(lane == 1, middle, jnp.where(lane == 2, low, 0.0)))
        return split.astype(jnp.bfloat16)

    def turned(split, first, chunk):
        place, other = selector((STAT, HEAD_DIM), 0, chunk)
        pick = jnp.where((place == other) & (other < 3), 1.0, 0.0).astype(jnp.bfloat16)
        return lax.dot_general(
            pick, split[first:first + HEAD_DIM], (((1,), (1,)), ((), ())), preferred_element_type=jnp.float32
        )

    def level_of(stats, chunk):
        place, _ = selector((STAT, HEAD_DIM), 0, chunk)
        ones = jnp.where((place >= 0) & (place < 3), 1.0, 0.0).astype(jnp.bfloat16)
        return lax.dot_general(stats, ones, (((0,), (0,)), ((), ())), preferred_element_type=jnp.float32)

    def hand_over(g, where):
        def finish(top, total, acc):
            result = (acc / total).astype(jnp.bfloat16)
            split = packed(top, total)
            for a in range(2):
                part_out[g, where, a, 0:half, :] = result[a * half:(a + 1) * half]
                stats = turned(split, a * half, 0) + turned(split, a * half + HEAD_DIM, 1)
                part_out[g, where, a, half:half + STAT, :] = stats.astype(jnp.bfloat16)
        return finish

    def hand_out(where):
        def finish(top, total, acc):
            result = (acc / total).astype(jnp.bfloat16)
            split = packed(top, total)
            for u in range(n_uly):
                last_out[where, u, 0:tokens, :] = result[u * tokens:(u + 1) * tokens]
                last_out[where, u, tokens:tokens + STAT, :] = turned(split, u * tokens, 0).astype(jnp.bfloat16)
        return finish

    def send_last(where, far, block=None):
        for d in (3, 2, 1, 0):
            src, dst = last_out.at[where, peers[d]], last_in.at[1 if far else 0, t]
            if d == 0 and not far:
                pltpu.make_async_copy(src, dst, last_own).start()
                continue
            place = {"uly": peers[d]} if block is None else {"seq": block, "uly": peers[d]}
            pltpu.make_async_remote_copy(
                src, dst, last_send, last_far.at[t] if far else last_own, device_id=place, device_id_type=MESH
            ).start()

    def join_last():
        landed(last_in.at[0], last_own)
        for d in range(n_uly):
            u = peers[d]
            landed(last_in.at[1, u], last_far.at[u])
            mine = level_of(last_in[0, u, tokens:tokens + STAT, :], 0)
            theirs = level_of(last_in[1, u, tokens:tokens + STAT, :], 0)
            top = jnp.maximum(mine, theirs)
            mine, theirs = jnp.exp2(mine - top), jnp.exp2(theirs - top)
            first = last_in[0, u, 0:tokens, :].astype(jnp.float32)
            second = last_in[1, u, 0:tokens, :].astype(jnp.float32)
            both = (first * mine + second * theirs) / (mine + theirs)
            back[:, columns(u, group - 1)] = both.astype(jnp.bfloat16)
        landed(back.at[:, 0:(group - 1) * n_uly * HEAD_DIM], back_sem)

    def merge(g, slot, a, lane=0):
        landed(part_in.at[slot, a], part_recv.at[slot, a])
        stats = part_in[slot, a, half:half + STAT, :]
        for chunk in range(2):
            level = level_of(stats, chunk)
            first = pl.multiple_of(a * half + chunk * HEAD_DIM, HEAD_DIM)
            cut = pl.ds(first, HEAD_DIM)
            top, total = own_stat[slot, 0, cut, :], own_stat[slot, 1, cut, :]
            new_top = jnp.maximum(top, level)
            mine, theirs = jnp.exp2(top - new_top), jnp.exp2(level - new_top)
            inverse = 1.0 / (total * mine + theirs)
            other = part_in[slot, a, chunk * HEAD_DIM:(chunk + 1) * HEAD_DIM, :].astype(jnp.float32)
            both = own[slot, cut, :] * (mine * inverse) + other * (theirs * inverse)
            att[lane, g, cut, :] = both.astype(jnp.bfloat16)

    def join(g, slot=None, lane=0):
        slot = g if slot is None else slot
        merge(g, slot, 1 - y, lane)
        give_back(g, (3, 2), lane)
        merge(g, slot, y, lane)
        give_back(g, (1, 0), lane)

    def each(first, count, body):
        def step(g, carry):
            body(g)
            return carry
        lax.fori_loop(first, count, step, 0)

    def add_up():
        past_load.wait()
        weights = [table_ref[0, slot_ref[p]] + table_ref[1, slot_ref[p]] for p in range(past.shape[0])]

        def sum_columns(uly):
            cols = pl.ds(pl.multiple_of(uly * (group * HEAD_DIM), HEAD_DIM), group * HEAD_DIM)
            mixed = weights[0] * past[0, :, cols].astype(jnp.float32)
            for p in range(1, past.shape[0]):
                mixed = mixed + weights[p] * past[p, :, cols].astype(jnp.float32)
            base_ref[:, cols] = mixed
        each(0, n_uly, sum_columns)

    def plane_sent():
        landed(given.at[:, :, 0:(n_uly - 1) * group * HEAD_DIM], plane_send)

    def line_sent(kind, block, first=0, count=group):
        landed(heads.at[kind, first:count, block], line_send.at[kind])

    def att_sent(first=0, count=group):
        if count > first:
            landed(att.at[0, first:count, 0:(n_uly - 1) * tokens, :], att_send.at[0])

    @pl.when(s == 0)
    def _():
        for kind in (K, V):
            pass_on(kind, 0, 0, 0, 1)
        order = [(kind, g) for g in range(group) for kind in (K, V)]
        for i, (kind, g) in enumerate(order):
            scatter(kind, g, i if g == 0 else None)
        for g in range(group):
            scatter(Q, g)
        for i, (kind, g) in enumerate(order):
            if i + 2 < len(order):
                pass_on(*order[i + 2], 0, 0, 1)
            forward(kind, g, 0, 1, i if g == 0 else None)
        for i in range(2):
            gathered_piece(*order[i], 0, i)
        add_up()

        def work(g):
            gathered(Q, g)
            attend(g, 0, (), True, settle(g))
            give_back(g, (3, 2, 1, 0))
        each(0, group, work)
        plane_sent()
        for kind in (K, V):
            line_sent(kind, 0)
        att_sent()
        landed(back, back_sem)

    @pl.when(s == 1)
    def _():
        for g in range(group):
            for kind in (K, V, Q):
                scatter(kind, g)
        add_up()

        def nearest(g):
            for kind in (K, V):
                gathered(kind, g)
            for block in (2, 3):
                arrived(Q, g, block)
                attend(g, block, (1,), False, keep(block - 2))
            for kind in (K, V):
                arrived(kind, g, 0)

        def near(g):
            gathered(Q, g)
            attend(g, 1, (0,), True, settle(g))
            give_back(g, (3, 2, 1, 0))

        def work(g):
            nearest(g)
            stays = g < len(guests)
            attend(g, 3, (0,), False, hand_over(g, 1), 1)
            for a in (1 - y, y):
                partial(g, 1, a, jnp.where(stays, 2, 3), jnp.where(stays, visit + g, g))
            attend(g, 2, (0,), False, hand_over(g, 0), 0)
            for a in (1 - y, y):
                partial(g, 0, a, 2, g)
            near(g)
        each(0, group - 1, work)
        nearest(group - 1)
        for block in (3, 2):
            attend(group - 1, block, (0,), False, hand_out(block - 2), block - 2)
            send_last(block - 2, True, block)
        near(group - 1)
        plane_sent()
        landed(part_out, part_send)
        landed(last_out, last_send)
        att_sent()
        landed(back, back_sem)

    @pl.when(s == 2)
    def _():
        pass_on(Q, 0, 0, 2, 1)
        for kind in (K, V):
            pass_on(kind, hosts[0], 0, 2, 3)
        order = [(Q, 0), (Q, 1)]
        for g in hosts:
            order += [(K, g), (V, g)] + ([(Q, g)] if g > 1 else [])
        order += [(Q, g) for g in range(2, hosts[0])]
        for kind, g in order:
            scatter(kind, g, g if kind == Q and g < 2 else None)
        for g in guests:
            for kind in (K, V):
                scatter(kind, g)
        for kind, g in order:
            to = 1 if kind == Q else 3
            if (g > 0 if kind == Q else g > hosts[0]):
                pass_on(kind, g, 0, 2, to)
            forward(kind, g, 2, to, g if kind == Q and g < 2 else None)
            if kind == Q and g > 0:
                relay(g)
        for g in range(2):
            gathered_piece(Q, g, 0, g)
        add_up()

        def near(g):
            attend(g, 2, (), True, keep(g))

        def own_guest(g):
            for kind in (K, V):
                gathered(kind, g)
            near(g)

        def receive(g):
            if g == 0:
                arrived(Q, g, 3)
            for kind in (K, V):
                arrived(kind, g, 3)
            attend(g, 3, (2,), True, keep(visit + g))

        attend(group - 1, 2, (), True, hand_out(0))
        send_last(0, False)
        each(hosts[0], group - 1, near)
        each(0, len(guests), own_guest)
        receive(0)
        join(0)
        join(0, visit, 1)
        for g in guests[1:]:
            join(g)
            receive(g)
            join(g, visit + g, 1)
        each(hosts[0], group - 1, join)
        plane_sent()
        line_sent(Q, 2)
        for kind in (K, V):
            line_sent(kind, 2, hosts[0])
        landed(heads.at[Q, 1:, 3], extra_send)
        landed(last_out.at[0, 0:n_uly - 1], last_send)
        landed(att.at[1, 0:len(guests)], att_send.at[1])
        att_sent(0, group - 1)
        join_last()

    @pl.when(s == 3)
    def _():
        pass_on(Q, 0, 0, 3, 1)
        pass_on(Q, 1, 0, 3, 2)
        for g in range(group):
            scatter(Q, g, g if g < 2 else None)
        for g in (*guests, *hosts):
            for kind in (K, V):
                scatter(kind, g)
        for g in range(group):
            if g > 1:
                pass_on(Q, g, 0, 3, 2)
            forward(Q, g, 3, 2 if g > 0 else 1, g if g < 2 else None)
        for d in range(n_uly):
            pass_on(Q, 0, d, 3, 2, extra_send)
        for g in guests:
            for kind in (K, V):
                pass_on(kind, g, 0, 3, 2)
                forward(kind, g, 3, 2)
        for g in range(2):
            gathered_piece(Q, g, 0, g)
        add_up()

        def near(g, finish=None):
            for kind in (K, V):
                gathered(kind, g)
                arrived(kind, g, 2)
            attend(g, 3, (2,), True, keep(g) if finish is None else finish)
        each(hosts[0], group - 1, near)
        near(group - 1, hand_out(0))
        send_last(0, False)
        each(hosts[0], group - 1, join)
        plane_sent()
        line_sent(Q, 3)
        for kind in (K, V):
            line_sent(kind, 3, 0, len(guests))
        landed(heads.at[Q, 0, 3], extra_send)
        landed(last_out.at[0, 0:n_uly - 1], last_send)
        att_sent(hosts[0], group - 1)
        join_last()


def fused(queries, keys, values, past_outputs, dwa_slot, dwa_table):
    n_seq, n_uly = lax.axis_size("seq"), lax.axis_size("uly")
    tokens, features = queries.shape
    group = features // n_uly // HEAD_DIM
    rows = tokens * n_uly
    slots = group + max(1, group // 2)
    stored = past_outputs.shape[0]
    bf16, f32 = jnp.bfloat16, jnp.float32
    anywhere = pl.BlockSpec(memory_space=pltpu.HBM)
    scalars = pl.BlockSpec(memory_space=pltpu.SMEM)
    attended, base = pl.pallas_call(
        functools.partial(fused_kernel, (n_seq, n_uly, group)),
        out_shape=(pltpu.VMEM((tokens, features), bf16), pltpu.VMEM((tokens, features), f32)),
        in_specs=[scalars, scalars, anywhere, anywhere, anywhere, anywhere],
        out_specs=[pl.BlockSpec(memory_space=pltpu.VMEM)] * 2,
        scratch_shapes=[
            pltpu.VMEM((3, tokens, features), bf16),
            pltpu.VMEM((stored, tokens, features), bf16),
            pltpu.VMEM((3, group, n_seq, rows, HEAD_DIM), bf16),
            pltpu.VMEM((slots, rows, HEAD_DIM), f32),
            pltpu.VMEM((slots, 2, rows, HEAD_DIM), f32),
            pltpu.VMEM((group - 1, 2, 2, rows // 2 + STAT, HEAD_DIM), bf16),
            pltpu.VMEM((slots, 2, rows // 2 + STAT, HEAD_DIM), bf16),
            pltpu.VMEM((2, group, rows, HEAD_DIM), bf16),
            pltpu.VMEM((2, n_uly, tokens + STAT, HEAD_DIM), bf16),
            pltpu.VMEM((2, n_uly, tokens + STAT, HEAD_DIM), bf16),
            pltpu.SemaphoreType.DMA,
            pltpu.SemaphoreType.DMA,
            pltpu.SemaphoreType.DMA,
            pltpu.SemaphoreType.DMA((2, n_uly)),
            pltpu.SemaphoreType.DMA((n_uly,)),
            pltpu.SemaphoreType.DMA((3, group)),
            pltpu.SemaphoreType.DMA((3,)),
            pltpu.SemaphoreType.DMA,
            pltpu.SemaphoreType.DMA((4, group)),
            pltpu.SemaphoreType.DMA,
            pltpu.SemaphoreType.DMA((slots, 2)),
            pltpu.SemaphoreType.DMA((2,)),
            pltpu.SemaphoreType.DMA,
            pltpu.SemaphoreType.DMA,
            pltpu.SemaphoreType.DMA,
            pltpu.SemaphoreType.DMA((n_uly,)),
        ],
        compiler_params=pltpu.CompilerParams(
            collective_id=0, has_side_effects=True, vmem_limit_bytes=32 * 1024 * 1024
        ),
    )(*(pltpu.with_memory_space_constraint(x, pltpu.HBM) for x in (dwa_slot, dwa_table, queries, keys, values, past_outputs)))
    return (base + attended.astype(f32)).astype(bf16)


def solution(mesh):
    def body(queries, *rest):
        heads_here = queries.shape[1] // HEAD_DIM // mesh.shape["uly"]
        fits = mesh.shape["seq"] == SPAN and mesh.shape["uly"] == PLANE and heads_here >= 2
        return (fused if fits else shards)(queries, *rest)

    return jax.shard_map(
        body,
        mesh=mesh,
        in_specs=(
            P(("rep", "seq", "uly"), None),
            P(("rep", "seq", "uly"), None),
            P(("rep", "seq", "uly"), None),
            P(None, ("rep", "seq", "uly"), None),
            P(),
            P(),
        ),
        out_specs=P(("rep", "seq", "uly"), None),
        check_vma=False,
    )
```

```python
import functools
import math

import jax
import jax.numpy as jnp
from jax import lax
from jax.experimental import pallas as pl
from jax.experimental.pallas import tpu as pltpu
from jax.sharding import PartitionSpec as P

HEAD_DIM = 128
SPAN = 4
PLANE = 4
STAT = 8
MESH = pl.DeviceIdType.MESH
Q, K, V = 0, 1, 2


def from_behind(block, axis, distance):
    devices = range(lax.axis_size(axis))
    route = [(i - distance, i) for i in devices if i - distance in devices]
    return lax.ppermute(block, axis, route)


def block_update(state, query_heads, key_heads, value_heads, allowed):
    running, total, accumulated = state
    scores = jnp.einsum("qhd,khd->hqk", query_heads, key_heads, preferred_element_type=jnp.float32)
    scores = scores * (1.0 / HEAD_DIM**0.5)
    scores = jnp.where(allowed, scores, -jnp.inf)
    new_max = jnp.maximum(running, jnp.max(scores, axis=2))
    factor = jnp.exp(running - new_max)
    prob = jnp.exp(scores - new_max[:, :, None])
    total = total * factor + jnp.sum(prob, axis=2)
    weights = prob.astype(jnp.bfloat16)
    update = jnp.einsum("hqk,khd->qhd", weights, value_heads, preferred_element_type=jnp.float32)
    accumulated = accumulated * jnp.transpose(factor)[:, :, None] + update
    return (new_max, total, accumulated)


def shards(queries, keys, values, past_outputs, dwa_slot, dwa_table):
    n_uly = lax.axis_size("uly")
    n_seq = lax.axis_size("seq")
    span_size = min(4, n_seq)
    features = queries.shape[1]
    local_heads = features // n_uly // HEAD_DIM
    query_rows, key_rows, value_rows = (
        lax.all_to_all(queries, "uly", split_axis=1, concat_axis=0, tiled=True),
        lax.all_to_all(keys, "uly", split_axis=1, concat_axis=0, tiled=True),
        lax.all_to_all(values, "uly", split_axis=1, concat_axis=0, tiled=True),
    )
    row_count = query_rows.shape[0]
    split_shape = (row_count, local_heads, HEAD_DIM)
    query_heads = query_rows.reshape(split_shape)
    table_index = jnp.arange(dwa_table.shape[1])
    onehot = (dwa_slot[:, None] == table_index[None, :]).astype(jnp.float32)
    coefs = jnp.dot(onehot, jnp.transpose(dwa_table), precision=lax.Precision.HIGHEST)
    layer_in = jnp.zeros(queries.shape, jnp.float32)
    extra = jnp.zeros(queries.shape, jnp.float32)
    for index in range(past_outputs.shape[0]):
        stored = past_outputs[index].astype(jnp.float32)
        layer_in = layer_in + coefs[index, 0] * stored
        extra = extra + coefs[index, 1] * stored
    running = jnp.full((local_heads, row_count), -jnp.inf, jnp.float32)
    total = jnp.zeros((local_heads, row_count), jnp.float32)
    accumulated = jnp.zeros(split_shape, jnp.float32)
    state = (running, total, accumulated)
    causal = (jnp.arange(row_count)[:, None] >= jnp.arange(row_count)[None, :])[None, :, :]
    state = block_update(
        state, query_heads, key_rows.reshape(split_shape), value_rows.reshape(split_shape), causal
    )
    position = lax.axis_index("seq")
    current = (key_rows, value_rows)
    for offset in range(1, span_size):
        current = from_behind((current[0], current[1]), "seq", 1)
        far_keys = current[0].reshape(split_shape)
        far_values = current[1].reshape(split_shape)

        def take_block(carry, far_keys=far_keys, far_values=far_values):
            return block_update(carry, query_heads, far_keys, far_values, True)

        def keep_block(carry):
            return carry

        state = lax.cond(position >= offset, take_block, keep_block, state)
    running, total, accumulated = state
    attended = accumulated / jnp.transpose(total)[:, :, None]
    attended = attended.astype(jnp.bfloat16).reshape(row_count, local_heads * HEAD_DIM)
    returned = lax.all_to_all(attended, "uly", split_axis=0, concat_axis=1, tiled=True)
    hidden = layer_in + returned.astype(jnp.float32)
    return (hidden + extra).astype(jnp.bfloat16)


def fused_kernel(
    shape,
    slot_hbm, table_hbm, q_hbm, k_hbm, v_hbm, past_hbm, back, base_ref,
    slot_ref, table_ref, given, past, heads, own, own_stat, part_out, part_in, att, last_out, last_in,
    load_sem, past_sem, table_sem, plane_send, piece_sem, relay_sem, whole_sem, line_send, extra_send, line_recv,
    part_send, part_recv, att_send, back_sem, last_send, last_own, last_far,
):
    n_seq, n_uly, group = shape
    tokens = given.shape[1]
    rows = n_uly * tokens
    half = rows // 2
    scale = math.log2(math.e) / HEAD_DIM**0.5
    s, t = lax.axis_index("seq"), lax.axis_index("uly")
    y, x = t // 2, t % 2
    peers = (t, 2 * y + 1 - x, 2 * (1 - y) + x, 3 - t)
    guests = range(max(1, group // 2))
    hosts = range(len(guests), group)
    visit = group
    lanes = {(Q, 2): 0, (Q, 3): 1, (K, 0): 2, (V, 0): 3, (K, 2): 2, (V, 2): 3, (K, 3): 2, (V, 3): 3}

    loads = [
        pltpu.make_async_copy(src, given.at[i], load_sem) for i, src in enumerate((q_hbm, k_hbm, v_hbm))
    ]
    table_loads = [
        pltpu.make_async_copy(src, dst, table_sem.at[i])
        for i, (src, dst) in enumerate(((slot_hbm, slot_ref), (table_hbm, table_ref)))
    ]
    past_load = pltpu.make_async_copy(past_hbm, past, past_sem)
    for load in (*loads, past_load, *table_loads):
        load.start()

    def landed(ref, sem):
        pltpu.make_async_copy(ref, ref, sem).wait()

    barrier = pltpu.get_barrier_semaphore()
    for d in (1, 2, 3):
        pl.semaphore_signal(barrier, inc=1, device_id={"uly": peers[d]}, device_id_type=MESH)
    neighbours = {0: (1,), 1: (0, 2, 3), 2: (1, 3), 3: (1, 2)}
    for place, others in neighbours.items():
        @pl.when(s == place)
        def _(place=place, others=others):
            for other in others:
                pl.semaphore_signal(barrier, inc=1, device_id={"seq": other}, device_id_type=MESH)
            if place == 3:
                for d in (1, 2, 3):
                    pl.semaphore_signal(barrier, inc=1, device_id={"seq": 2, "uly": peers[d]}, device_id_type=MESH)
            pl.semaphore_wait(barrier, 3 + len(others) + (3 if place == 2 else 0))
    landed(given, load_sem)

    def columns(uly, g):
        return pl.ds(pl.multiple_of((uly * group + g) * HEAD_DIM, HEAD_DIM), HEAD_DIM)

    def row_range(uly):
        return pl.ds(pl.multiple_of(uly * tokens, tokens), tokens)

    def scatter(kind, g, pieces=None):
        for d in (1, 2, 3, 0):
            src = given.at[kind, :, columns(peers[d], g)]
            dst = heads.at[kind, g, s, row_range(t), :]
            sem = whole_sem.at[kind, g] if pieces is None else piece_sem.at[pieces, d]
            if d == 0:
                pltpu.make_async_copy(src, dst, sem).start()
            else:
                pltpu.make_async_remote_copy(
                    src, dst, plane_send, sem, device_id={"uly": peers[d]}, device_id_type=MESH
                ).start()

    def gathered(kind, g):
        landed(heads.at[kind, g, s], whole_sem.at[kind, g])

    def gathered_piece(kind, g, d, pieces):
        landed(heads.at[kind, g, s, row_range(peers[d]), :], piece_sem.at[pieces, d])

    def arrived(kind, g, block):
        landed(heads.at[kind, g, block], line_recv.at[lanes[kind, block], g])

    def pass_on(kind, g, d, block, to):
        dst = heads.at[kind, g, block, row_range(peers[d]), :]
        src = given.at[kind, :, columns(t, g)] if d == 0 else dst
        piecewise = kind == Q and block == 3 and g < 2
        sem = relay_sem.at[g, d] if piecewise else line_recv.at[lanes[kind, block], g]
        pltpu.make_async_remote_copy(
            src, dst, line_send.at[kind], sem,
            device_id={"seq": to}, device_id_type=MESH,
        ).start()

    def forward(kind, g, block, to, pieces=None):
        if pieces is None:
            gathered(kind, g)
        for d in (1, 2, 3):
            if pieces is not None:
                gathered_piece(kind, g, d, pieces)
            pass_on(kind, g, d, block, to)

    def relay(g):
        parts = [heads.at[Q, g, 3]]
        if g < 2:
            parts = [heads.at[Q, g, 3, row_range(peers[d]), :] for d in range(n_uly)]
        for d, ref in enumerate(parts):
            landed(ref, relay_sem.at[g, d] if g < 2 else line_recv.at[lanes[Q, 3], g])
            pltpu.make_async_remote_copy(
                ref, ref, extra_send, line_recv.at[lanes[Q, 3], g], device_id={"seq": 1}, device_id_type=MESH
            ).start()

    def partial(g, where, a, to, slot):
        pltpu.make_async_remote_copy(
            part_out.at[g, where, a], part_in.at[slot, a], part_send, part_recv.at[slot, a],
            device_id={"seq": to}, device_id_type=MESH,
        ).start()

    def give_back(g, ds, lane=0):
        for d in ds:
            src = att.at[lane, g, row_range(peers[d]), :]
            dst = back.at[:, columns(t, g)]
            if lane == 0 and d == 0:
                pltpu.make_async_copy(src, dst, back_sem).start()
                continue
            where = {"uly": peers[d]} if lane == 0 else {"seq": n_seq - 1, "uly": peers[d]}
            pltpu.make_async_remote_copy(
                src, dst, att_send.at[lane], back_sem, device_id=where, device_id_type=MESH
            ).start()

    def attend(g, block, full, diagonal, finish, resume=None):
        query = heads[Q, g, block]
        acc_shape = (rows, HEAD_DIM)
        top = total = acc = None
        if resume is not None:
            top, total, acc = own_stat[resume, 0], own_stat[resume, 1], own[resume]
        for j in (*full, block) if diagonal else full:
            key = heads[K, g, j]
            value = heads[V, g, j]
            scores = lax.dot_general(query, key, (((1,), (1,)), ((), ())), preferred_element_type=jnp.float32)
            scores = scores * scale
            if j == block:
                query_at = lax.broadcasted_iota(jnp.int32, scores.shape, 0)
                key_at = lax.broadcasted_iota(jnp.int32, scores.shape, 1)
                scores = jnp.where(key_at <= query_at, scores, -jnp.inf)
            peak = jnp.broadcast_to(jnp.max(scores, axis=1, keepdims=True), acc_shape)
            new_top = peak if top is None else jnp.maximum(top, peak)
            prob = jnp.exp2(scores - jnp.concatenate([new_top] * (rows // HEAD_DIM), axis=1))
            sums = jnp.broadcast_to(jnp.sum(prob, axis=1, keepdims=True), acc_shape)
            update = jnp.dot(prob.astype(jnp.bfloat16), value, preferred_element_type=jnp.float32)
            if top is None:
                total, acc = sums, update
            else:
                factor = jnp.exp2(top - new_top)
                total = total * factor + sums
                acc = acc * factor + update
            top = new_top
        finish(top, total, acc)

    def settle(g):
        def finish(top, total, acc):
            att[0, g] = (acc / total).astype(jnp.bfloat16)
        return finish

    def keep(slot):
        def finish(top, total, acc):
            own[slot] = acc
            own_stat[slot, 0] = top
            own_stat[slot, 1] = total
        return finish

    def selector(shape, dim, chunk):
        place = lax.broadcasted_iota(jnp.int32, shape, dim) - 3 * chunk
        other = lax.broadcasted_iota(jnp.int32, shape, 1 - dim)
        return place, other

    def packed(top, total):
        level = top + jnp.log2(total)
        high = level.astype(jnp.bfloat16).astype(jnp.float32)
        middle = (level - high).astype(jnp.bfloat16).astype(jnp.float32)
        low = level - high - middle
        lane = lax.broadcasted_iota(jnp.int32, (rows, HEAD_DIM), 1)
        split = jnp.where(lane == 0, high, jnp.where(lane == 1, middle, jnp.where(lane == 2, low, 0.0)))
        return split.astype(jnp.bfloat16)

    def turned(split, first, chunk):
        place, other = selector((STAT, HEAD_DIM), 0, chunk)
        pick = jnp.where((place == other) & (other < 3), 1.0, 0.0).astype(jnp.bfloat16)
        return lax.dot_general(
            pick, split[first:first + HEAD_DIM], (((1,), (1,)), ((), ())), preferred_element_type=jnp.float32
        )

    def level_of(stats, chunk):
        place, _ = selector((STAT, HEAD_DIM), 0, chunk)
        ones = jnp.where((place >= 0) & (place < 3), 1.0, 0.0).astype(jnp.bfloat16)
        return lax.dot_general(stats, ones, (((0,), (0,)), ((), ())), preferred_element_type=jnp.float32)

    def hand_over(g, where):
        def finish(top, total, acc):
            result = (acc / total).astype(jnp.bfloat16)
            split = packed(top, total)
            for a in range(2):
                part_out[g, where, a, 0:half, :] = result[a * half:(a + 1) * half]
                stats = turned(split, a * half, 0) + turned(split, a * half + HEAD_DIM, 1)
                part_out[g, where, a, half:half + STAT, :] = stats.astype(jnp.bfloat16)
        return finish

    def hand_out(where):
        def finish(top, total, acc):
            result = (acc / total).astype(jnp.bfloat16)
            split = packed(top, total)
            for u in range(n_uly):
                last_out[where, u, 0:tokens, :] = result[u * tokens:(u + 1) * tokens]
                last_out[where, u, tokens:tokens + STAT, :] = turned(split, u * tokens, 0).astype(jnp.bfloat16)
        return finish

    def send_last(where, far, block=None):
        for d in (3, 2, 1, 0):
            src, dst = last_out.at[where, peers[d]], last_in.at[1 if far else 0, t]
            if d == 0 and not far:
                pltpu.make_async_copy(src, dst, last_own).start()
                continue
            place = {"uly": peers[d]} if block is None else {"seq": block, "uly": peers[d]}
            pltpu.make_async_remote_copy(
                src, dst, last_send, last_far.at[t] if far else last_own, device_id=place, device_id_type=MESH
            ).start()

    def join_last():
        landed(last_in.at[0], last_own)
        for d in range(n_uly):
            u = peers[d]
            landed(last_in.at[1, u], last_far.at[u])
            mine = level_of(last_in[0, u, tokens:tokens + STAT, :], 0)
            theirs = level_of(last_in[1, u, tokens:tokens + STAT, :], 0)
            top = jnp.maximum(mine, theirs)
            mine, theirs = jnp.exp2(mine - top), jnp.exp2(theirs - top)
            first = last_in[0, u, 0:tokens, :].astype(jnp.float32)
            second = last_in[1, u, 0:tokens, :].astype(jnp.float32)
            both = (first * mine + second * theirs) / (mine + theirs)
            back[:, columns(u, group - 1)] = both.astype(jnp.bfloat16)
        landed(back.at[:, 0:(group - 1) * n_uly * HEAD_DIM], back_sem)

    def merge(g, slot, a, lane=0):
        landed(part_in.at[slot, a], part_recv.at[slot, a])
        stats = part_in[slot, a, half:half + STAT, :]
        for chunk in range(2):
            level = level_of(stats, chunk)
            first = pl.multiple_of(a * half + chunk * HEAD_DIM, HEAD_DIM)
            cut = pl.ds(first, HEAD_DIM)
            top, total = own_stat[slot, 0, cut, :], own_stat[slot, 1, cut, :]
            new_top = jnp.maximum(top, level)
            mine, theirs = jnp.exp2(top - new_top), jnp.exp2(level - new_top)
            inverse = 1.0 / (total * mine + theirs)
            other = part_in[slot, a, chunk * HEAD_DIM:(chunk + 1) * HEAD_DIM, :].astype(jnp.float32)
            both = own[slot, cut, :] * (mine * inverse) + other * (theirs * inverse)
            att[lane, g, cut, :] = both.astype(jnp.bfloat16)

    def join(g, slot=None, lane=0):
        slot = g if slot is None else slot
        merge(g, slot, 1 - y, lane)
        give_back(g, (3, 2), lane)
        merge(g, slot, y, lane)
        give_back(g, (1, 0), lane)

    def each(first, count, body):
        def step(g, carry):
            body(g)
            return carry
        lax.fori_loop(first, count, step, 0)

    def add_up():
        for load in (past_load, *table_loads):
            load.wait()
        weights = [table_ref[0, slot_ref[p]] + table_ref[1, slot_ref[p]] for p in range(past.shape[0])]

        def sum_columns(uly):
            cols = pl.ds(pl.multiple_of(uly * (group * HEAD_DIM), HEAD_DIM), group * HEAD_DIM)
            mixed = weights[0] * past[0, :, cols].astype(jnp.float32)
            for p in range(1, past.shape[0]):
                mixed = mixed + weights[p] * past[p, :, cols].astype(jnp.float32)
            base_ref[:, cols] = mixed
        each(0, n_uly, sum_columns)

    def plane_sent():
        landed(given.at[:, :, 0:(n_uly - 1) * group * HEAD_DIM], plane_send)

    def line_sent(kind, block, first=0, count=group):
        landed(heads.at[kind, first:count, block], line_send.at[kind])

    def att_sent(first=0, count=group):
        if count > first:
            landed(att.at[0, first:count, 0:(n_uly - 1) * tokens, :], att_send.at[0])

    @pl.when(s == 0)
    def _():
        for kind in (K, V):
            pass_on(kind, 0, 0, 0, 1)
        order = [(kind, g) for g in range(group) for kind in (K, V)]
        for i, (kind, g) in enumerate(order):
            scatter(kind, g, i if g == 0 else None)
        for g in range(group):
            scatter(Q, g)
        for i, (kind, g) in enumerate(order):
            if i + 2 < len(order):
                pass_on(*order[i + 2], 0, 0, 1)
            forward(kind, g, 0, 1, i if g == 0 else None)
        for i in range(2):
            gathered_piece(*order[i], 0, i)
        add_up()

        def work(g):
            gathered(Q, g)
            attend(g, 0, (), True, settle(g))
            give_back(g, (3, 2, 1, 0))
        each(0, group, work)
        plane_sent()
        for kind in (K, V):
            line_sent(kind, 0)
        att_sent()
        landed(back, back_sem)

    @pl.when(s == 1)
    def _():
        for g in range(group):
            for kind in (K, V, Q):
                scatter(kind, g)
        add_up()

        def far(g, block, finish):
            if block == 2:
                for kind in (K, V):
                    gathered(kind, g)
            arrived(Q, g, block)
            attend(g, block, (1,), False, keep(block - 2))
            if block == 2:
                for kind in (K, V):
                    arrived(kind, g, 0)
            attend(g, block, (0,), False, finish, block - 2)

        def near(g):
            gathered(Q, g)
            attend(g, 1, (0,), True, settle(g))
            give_back(g, (3, 2, 1, 0))

        def work(g):
            far(g, 2, hand_over(g, 0))
            for a in (1 - y, y):
                partial(g, 0, a, 2, g)
            far(g, 3, hand_over(g, 1))
            stays = g < len(guests)
            for a in (1 - y, y):
                partial(g, 1, a, jnp.where(stays, 2, 3), jnp.where(stays, visit + g, g))
            near(g)
        each(0, group - 1, work)
        for block in (2, 3):
            far(group - 1, block, hand_out(block - 2))
            send_last(block - 2, True, block)
        near(group - 1)
        plane_sent()
        landed(part_out, part_send)
        landed(last_out, last_send)
        att_sent()
        landed(back, back_sem)

    @pl.when(s == 2)
    def _():
        pass_on(Q, 0, 0, 2, 1)
        for kind in (K, V):
            pass_on(kind, hosts[0], 0, 2, 3)
        order = [(Q, 0), (Q, 1)]
        for g in hosts:
            order += [(K, g), (V, g)] + ([(Q, g)] if g > 1 else [])
        order += [(Q, g) for g in range(2, hosts[0])]
        for kind, g in order:
            scatter(kind, g, g if kind == Q and g < 2 else None)
        for g in guests:
            for kind in (K, V):
                scatter(kind, g)
        for kind, g in order:
            to = 1 if kind == Q else 3
            if (g > 0 if kind == Q else g > hosts[0]):
                pass_on(kind, g, 0, 2, to)
            forward(kind, g, 2, to, g if kind == Q and g < 2 else None)
            if kind == Q:
                relay(g)
        for g in range(2):
            gathered_piece(Q, g, 0, g)
        add_up()

        def near(g):
            attend(g, 2, (), True, keep(g))

        def own_guest(g):
            for kind in (K, V):
                gathered(kind, g)
            near(g)

        def receive(g):
            for kind in (K, V):
                arrived(kind, g, 3)
            attend(g, 3, (2,), True, keep(visit + g))

        attend(group - 1, 2, (), True, hand_out(0))
        send_last(0, False)
        each(hosts[0], group - 1, near)
        each(0, len(guests), own_guest)
        receive(0)
        join(0)
        join(0, visit, 1)
        for g in guests[1:]:
            join(g)
            receive(g)
            join(g, visit + g, 1)
        each(hosts[0], group - 1, join)
        plane_sent()
        line_sent(Q, 2)
        for kind in (K, V):
            line_sent(kind, 2, hosts[0])
        landed(heads.at[Q, :, 3], extra_send)
        landed(last_out.at[0, 0:n_uly - 1], last_send)
        landed(att.at[1, 0:len(guests)], att_send.at[1])
        att_sent(0, group - 1)
        join_last()

    @pl.when(s == 3)
    def _():
        for g in range(2):
            pass_on(Q, g, 0, 3, 2)
        for g in range(group):
            scatter(Q, g, g if g < 2 else None)
        for g in (*guests, *hosts):
            for kind in (K, V):
                scatter(kind, g)
        for g in range(group):
            if g > 1:
                pass_on(Q, g, 0, 3, 2)
            forward(Q, g, 3, 2, g if g < 2 else None)
        for g in guests:
            for kind in (K, V):
                pass_on(kind, g, 0, 3, 2)
                forward(kind, g, 3, 2)
        for g in range(2):
            gathered_piece(Q, g, 0, g)
        add_up()

        def near(g, finish=None):
            for kind in (K, V):
                gathered(kind, g)
                arrived(kind, g, 2)
            attend(g, 3, (2,), True, keep(g) if finish is None else finish)
        each(hosts[0], group - 1, near)
        near(group - 1, hand_out(0))
        send_last(0, False)
        each(hosts[0], group - 1, join)
        plane_sent()
        line_sent(Q, 3)
        for kind in (K, V):
            line_sent(kind, 3, 0, len(guests))
        landed(last_out.at[0, 0:n_uly - 1], last_send)
        att_sent(hosts[0], group - 1)
        join_last()


def fused(queries, keys, values, past_outputs, dwa_slot, dwa_table):
    n_seq, n_uly = lax.axis_size("seq"), lax.axis_size("uly")
    tokens, features = queries.shape
    group = features // n_uly // HEAD_DIM
    rows = tokens * n_uly
    slots = group + max(1, group // 2)
    stored = past_outputs.shape[0]
    bf16, f32 = jnp.bfloat16, jnp.float32
    anywhere = pl.BlockSpec(memory_space=pltpu.HBM)
    attended, base = pl.pallas_call(
        functools.partial(fused_kernel, (n_seq, n_uly, group)),
        out_shape=(pltpu.VMEM((tokens, features), bf16), pltpu.VMEM((tokens, features), f32)),
        in_specs=[anywhere] * 6,
        out_specs=[pl.BlockSpec(memory_space=pltpu.VMEM)] * 2,
        scratch_shapes=[
            pltpu.SMEM(dwa_slot.shape, jnp.int32),
            pltpu.SMEM(dwa_table.shape, f32),
            pltpu.VMEM((3, tokens, features), bf16),
            pltpu.VMEM((stored, tokens, features), bf16),
            pltpu.VMEM((3, group, n_seq, rows, HEAD_DIM), bf16),
            pltpu.VMEM((slots, rows, HEAD_DIM), f32),
            pltpu.VMEM((slots, 2, rows, HEAD_DIM), f32),
            pltpu.VMEM((group - 1, 2, 2, rows // 2 + STAT, HEAD_DIM), bf16),
            pltpu.VMEM((slots, 2, rows // 2 + STAT, HEAD_DIM), bf16),
            pltpu.VMEM((2, group, rows, HEAD_DIM), bf16),
            pltpu.VMEM((2, n_uly, tokens + STAT, HEAD_DIM), bf16),
            pltpu.VMEM((2, n_uly, tokens + STAT, HEAD_DIM), bf16),
            pltpu.SemaphoreType.DMA,
            pltpu.SemaphoreType.DMA,
            pltpu.SemaphoreType.DMA((2,)),
            pltpu.SemaphoreType.DMA,
            pltpu.SemaphoreType.DMA((2, n_uly)),
            pltpu.SemaphoreType.DMA((2, n_uly)),
            pltpu.SemaphoreType.DMA((3, group)),
            pltpu.SemaphoreType.DMA((3,)),
            pltpu.SemaphoreType.DMA,
            pltpu.SemaphoreType.DMA((4, group)),
            pltpu.SemaphoreType.DMA,
            pltpu.SemaphoreType.DMA((slots, 2)),
            pltpu.SemaphoreType.DMA((2,)),
            pltpu.SemaphoreType.DMA,
            pltpu.SemaphoreType.DMA,
            pltpu.SemaphoreType.DMA,
            pltpu.SemaphoreType.DMA((n_uly,)),
        ],
        compiler_params=pltpu.CompilerParams(
            collective_id=0, has_side_effects=True, vmem_limit_bytes=32 * 1024 * 1024
        ),
    )(*(pltpu.with_memory_space_constraint(x, pltpu.HBM) for x in (dwa_slot, dwa_table, queries, keys, values, past_outputs)))
    return (base + attended.astype(f32)).astype(bf16)


def solution(mesh):
    def body(queries, *rest):
        heads_here = queries.shape[1] // HEAD_DIM // mesh.shape["uly"]
        fits = mesh.shape["seq"] == SPAN and mesh.shape["uly"] == PLANE and heads_here >= 2
        return (fused if fits else shards)(queries, *rest)

    return jax.shard_map(
        body,
        mesh=mesh,
        in_specs=(
            P(("rep", "seq", "uly"), None),
            P(("rep", "seq", "uly"), None),
            P(("rep", "seq", "uly"), None),
            P(None, ("rep", "seq", "uly"), None),
            P(),
            P(),
        ),
        out_specs=P(("rep", "seq", "uly"), None),
        check_vma=False,
    )
```

```python
import functools
import math

import jax
import jax.numpy as jnp
from jax import lax
from jax.experimental import pallas as pl
from jax.experimental.pallas import tpu as pltpu
from jax.sharding import PartitionSpec as P

HEAD_DIM = 128
SPAN = 4
PLANE = 4
STAT = 8
MESH = pl.DeviceIdType.MESH
Q, K, V = 0, 1, 2


def from_behind(block, axis, distance):
    devices = range(lax.axis_size(axis))
    route = [(i - distance, i) for i in devices if i - distance in devices]
    return lax.ppermute(block, axis, route)


def block_update(state, query_heads, key_heads, value_heads, allowed):
    running, total, accumulated = state
    scores = jnp.einsum("qhd,khd->hqk", query_heads, key_heads, preferred_element_type=jnp.float32)
    scores = scores * (1.0 / HEAD_DIM**0.5)
    scores = jnp.where(allowed, scores, -jnp.inf)
    new_max = jnp.maximum(running, jnp.max(scores, axis=2))
    factor = jnp.exp(running - new_max)
    prob = jnp.exp(scores - new_max[:, :, None])
    total = total * factor + jnp.sum(prob, axis=2)
    weights = prob.astype(jnp.bfloat16)
    update = jnp.einsum("hqk,khd->qhd", weights, value_heads, preferred_element_type=jnp.float32)
    accumulated = accumulated * jnp.transpose(factor)[:, :, None] + update
    return (new_max, total, accumulated)


def shards(queries, keys, values, past_outputs, dwa_slot, dwa_table):
    n_uly = lax.axis_size("uly")
    n_seq = lax.axis_size("seq")
    span_size = min(4, n_seq)
    features = queries.shape[1]
    local_heads = features // n_uly // HEAD_DIM
    query_rows, key_rows, value_rows = (
        lax.all_to_all(queries, "uly", split_axis=1, concat_axis=0, tiled=True),
        lax.all_to_all(keys, "uly", split_axis=1, concat_axis=0, tiled=True),
        lax.all_to_all(values, "uly", split_axis=1, concat_axis=0, tiled=True),
    )
    row_count = query_rows.shape[0]
    split_shape = (row_count, local_heads, HEAD_DIM)
    query_heads = query_rows.reshape(split_shape)
    table_index = jnp.arange(dwa_table.shape[1])
    onehot = (dwa_slot[:, None] == table_index[None, :]).astype(jnp.float32)
    coefs = jnp.dot(onehot, jnp.transpose(dwa_table), precision=lax.Precision.HIGHEST)
    layer_in = jnp.zeros(queries.shape, jnp.float32)
    extra = jnp.zeros(queries.shape, jnp.float32)
    for index in range(past_outputs.shape[0]):
        stored = past_outputs[index].astype(jnp.float32)
        layer_in = layer_in + coefs[index, 0] * stored
        extra = extra + coefs[index, 1] * stored
    running = jnp.full((local_heads, row_count), -jnp.inf, jnp.float32)
    total = jnp.zeros((local_heads, row_count), jnp.float32)
    accumulated = jnp.zeros(split_shape, jnp.float32)
    state = (running, total, accumulated)
    causal = (jnp.arange(row_count)[:, None] >= jnp.arange(row_count)[None, :])[None, :, :]
    state = block_update(
        state, query_heads, key_rows.reshape(split_shape), value_rows.reshape(split_shape), causal
    )
    position = lax.axis_index("seq")
    current = (key_rows, value_rows)
    for offset in range(1, span_size):
        current = from_behind((current[0], current[1]), "seq", 1)
        far_keys = current[0].reshape(split_shape)
        far_values = current[1].reshape(split_shape)

        def take_block(carry, far_keys=far_keys, far_values=far_values):
            return block_update(carry, query_heads, far_keys, far_values, True)

        def keep_block(carry):
            return carry

        state = lax.cond(position >= offset, take_block, keep_block, state)
    running, total, accumulated = state
    attended = accumulated / jnp.transpose(total)[:, :, None]
    attended = attended.astype(jnp.bfloat16).reshape(row_count, local_heads * HEAD_DIM)
    returned = lax.all_to_all(attended, "uly", split_axis=0, concat_axis=1, tiled=True)
    hidden = layer_in + returned.astype(jnp.float32)
    return (hidden + extra).astype(jnp.bfloat16)


def fused_kernel(
    shape,
    slot_hbm, table_hbm, q_hbm, k_hbm, v_hbm, past_hbm, back, base_ref,
    slot_ref, table_ref, given, past, heads, own, own_stat, part_out, part_in, att, last_out, last_in,
    load_sem, past_sem, table_sem, plane_send, piece_sem, relay_sem, whole_sem, line_send, extra_send, line_recv,
    part_send, part_recv, att_send, back_sem, last_send, last_own, last_far,
):
    n_seq, n_uly, group = shape
    tokens = given.shape[1]
    rows = n_uly * tokens
    half = rows // 2
    scale = math.log2(math.e) / HEAD_DIM**0.5
    s, t = lax.axis_index("seq"), lax.axis_index("uly")
    y, x = t // 2, t % 2
    ahead = lax.axis_index("rep") % 2 == 1
    behind = jnp.logical_not(ahead)
    peers = (t, 2 * y + 1 - x, 2 * (1 - y) + x, 3 - t)
    guests = range(max(1, group // 2))
    hosts = range(len(guests), group)
    visit = group - 1
    lanes = {(Q, 2): 0, (Q, 3): 1, (K, 0): 2, (V, 0): 2, (K, 2): 2, (V, 2): 2, (K, 3): 2, (V, 3): 2}

    loads = [
        pltpu.make_async_copy(src, given.at[i], load_sem) for i, src in enumerate((q_hbm, k_hbm, v_hbm))
    ]
    table_loads = [
        pltpu.make_async_copy(src, dst, table_sem.at[i])
        for i, (src, dst) in enumerate(((slot_hbm, slot_ref), (table_hbm, table_ref)))
    ]
    past_load = pltpu.make_async_copy(past_hbm, past, past_sem)
    for load in (*loads, past_load, *table_loads):
        load.start()

    def landed(ref, sem):
        pltpu.make_async_copy(ref, ref, sem).wait()

    barrier = pltpu.get_barrier_semaphore()
    for d in (1, 2, 3):
        pl.semaphore_signal(barrier, inc=1, device_id={"uly": peers[d]}, device_id_type=MESH)
    neighbours = {0: (1,), 1: (0, 2, 3), 2: (1, 3), 3: (1, 2)}
    for place, others in neighbours.items():
        @pl.when(s == place)
        def _(place=place, others=others):
            for other in others:
                pl.semaphore_signal(barrier, inc=1, device_id={"seq": other}, device_id_type=MESH)
            if place == 3:
                for d in (1, 2, 3):
                    pl.semaphore_signal(barrier, inc=1, device_id={"seq": 2, "uly": peers[d]}, device_id_type=MESH)
            pl.semaphore_wait(barrier, 3 + len(others) + (3 if place == 2 else 0))
    landed(given, load_sem)

    def columns(uly, g):
        return pl.ds(pl.multiple_of((uly * group + g) * HEAD_DIM, HEAD_DIM), HEAD_DIM)

    def row_range(uly):
        return pl.ds(pl.multiple_of(uly * tokens, tokens), tokens)

    def scatter(kind, g, pieces=None):
        for d in (1, 2, 3, 0):
            src = given.at[kind, :, columns(peers[d], g)]
            dst = heads.at[kind, g, s, row_range(t), :]
            sem = whole_sem.at[kind, g] if pieces is None else piece_sem.at[pieces, d]
            if d == 0:
                pltpu.make_async_copy(src, dst, sem).start()
            else:
                pltpu.make_async_remote_copy(
                    src, dst, plane_send, sem, device_id={"uly": peers[d]}, device_id_type=MESH
                ).start()

    def gathered(kind, g):
        landed(heads.at[kind, g, s], whole_sem.at[kind, g])

    def gathered_piece(kind, g, d, pieces):
        landed(heads.at[kind, g, s, row_range(peers[d]), :], piece_sem.at[pieces, d])

    def arrived(kind, g, block):
        ref = heads.at[Q, g, block] if kind == Q else heads.at[K:V + 1, g, block]
        landed(ref, line_recv.at[lanes[kind, block], g])

    def pass_on(kind, g, d, block, to):
        dst = heads.at[kind, g, block, row_range(peers[d]), :]
        src = given.at[kind, :, columns(t, g)] if d == 0 else dst
        piecewise = kind == Q and block == 3 and g < 2
        sem = relay_sem.at[g, d] if piecewise else line_recv.at[lanes[kind, block], g]
        pltpu.make_async_remote_copy(
            src, dst, line_send.at[kind], sem,
            device_id={"seq": to}, device_id_type=MESH,
        ).start()

    def forward(kind, g, block, to, pieces=None):
        if pieces is None:
            gathered(kind, g)
        for d in (1, 2, 3):
            if pieces is not None:
                gathered_piece(kind, g, d, pieces)
            pass_on(kind, g, d, block, to)

    def relay(g):
        parts = [heads.at[Q, g, 3]]
        if g < 2:
            parts = [heads.at[Q, g, 3, row_range(peers[d]), :] for d in range(n_uly)]
        for d, ref in enumerate(parts):
            landed(ref, relay_sem.at[g, d] if g < 2 else line_recv.at[lanes[Q, 3], g])
            pltpu.make_async_remote_copy(
                ref, ref, extra_send, line_recv.at[lanes[Q, 3], g], device_id={"seq": 1}, device_id_type=MESH
            ).start()

    def partial(g, where, a, to, slot):
        pltpu.make_async_remote_copy(
            part_out.at[g, where, a], part_in.at[slot, a], part_send, part_recv.at[slot, a],
            device_id={"seq": to}, device_id_type=MESH,
        ).start()

    def give_back(g, ds, lane=0):
        for d in ds:
            src = att.at[lane, g, row_range(peers[d]), :]
            dst = back.at[:, columns(t, g)]
            if lane == 0 and d == 0:
                pltpu.make_async_copy(src, dst, back_sem).start()
                continue
            where = {"uly": peers[d]} if lane == 0 else {"seq": n_seq - 1, "uly": peers[d]}
            pltpu.make_async_remote_copy(
                src, dst, att_send.at[lane], back_sem, device_id=where, device_id_type=MESH
            ).start()

    def attend(g, block, full, diagonal, finish, resume=None):
        query = heads[Q, g, block]
        acc_shape = (rows, HEAD_DIM)
        top = total = acc = None
        if resume is not None:
            top, total, acc = own_stat[resume, 0], own_stat[resume, 1], own[resume]
        for j in (*full, block) if diagonal else full:
            key = heads[K, g, j]
            value = heads[V, g, j]
            scores = lax.dot_general(query, key, (((1,), (1,)), ((), ())), preferred_element_type=jnp.float32)
            scores = scores * scale
            if j == block:
                query_at = lax.broadcasted_iota(jnp.int32, scores.shape, 0)
                key_at = lax.broadcasted_iota(jnp.int32, scores.shape, 1)
                scores = jnp.where(key_at <= query_at, scores, -jnp.inf)
            peak = jnp.broadcast_to(jnp.max(scores, axis=1, keepdims=True), acc_shape)
            new_top = peak if top is None else jnp.maximum(top, peak)
            prob = jnp.exp2(scores - jnp.concatenate([new_top] * (rows // HEAD_DIM), axis=1))
            sums = jnp.broadcast_to(jnp.sum(prob, axis=1, keepdims=True), acc_shape)
            update = jnp.dot(prob.astype(jnp.bfloat16), value, preferred_element_type=jnp.float32)
            if top is None:
                total, acc = sums, update
            else:
                factor = jnp.exp2(top - new_top)
                total = total * factor + sums
                acc = acc * factor + update
            top = new_top
        finish(top, total, acc)

    def settle(g):
        def finish(top, total, acc):
            att[0, g] = (acc / total).astype(jnp.bfloat16)
        return finish

    def keep(slot):
        def finish(top, total, acc):
            own[slot] = acc
            own_stat[slot, 0] = top
            own_stat[slot, 1] = total
        return finish

    def selector(shape, dim, chunk):
        place = lax.broadcasted_iota(jnp.int32, shape, dim) - 3 * chunk
        other = lax.broadcasted_iota(jnp.int32, shape, 1 - dim)
        return place, other

    def packed(top, total):
        level = top + jnp.log2(total)
        high = level.astype(jnp.bfloat16).astype(jnp.float32)
        middle = (level - high).astype(jnp.bfloat16).astype(jnp.float32)
        low = level - high - middle
        lane = lax.broadcasted_iota(jnp.int32, (rows, HEAD_DIM), 1)
        split = jnp.where(lane == 0, high, jnp.where(lane == 1, middle, jnp.where(lane == 2, low, 0.0)))
        return split.astype(jnp.bfloat16)

    def turned(split, first, chunk):
        place, other = selector((STAT, HEAD_DIM), 0, chunk)
        pick = jnp.where((place == other) & (other < 3), 1.0, 0.0).astype(jnp.bfloat16)
        return lax.dot_general(
            pick, split[first:first + HEAD_DIM], (((1,), (1,)), ((), ())), preferred_element_type=jnp.float32
        )

    def level_of(stats, chunk):
        place, _ = selector((STAT, HEAD_DIM), 0, chunk)
        ones = jnp.where((place >= 0) & (place < 3), 1.0, 0.0).astype(jnp.bfloat16)
        return lax.dot_general(stats, ones, (((0,), (0,)), ((), ())), preferred_element_type=jnp.float32)

    def hand_over(g, where):
        def finish(top, total, acc):
            result = (acc / total).astype(jnp.bfloat16)
            split = packed(top, total)
            for a in range(2):
                part_out[g, where, a, 0:half, :] = result[a * half:(a + 1) * half]
                stats = turned(split, a * half, 0) + turned(split, a * half + HEAD_DIM, 1)
                part_out[g, where, a, half:half + STAT, :] = stats.astype(jnp.bfloat16)
        return finish

    def hand_out(where):
        def finish(top, total, acc):
            result = (acc / total).astype(jnp.bfloat16)
            split = packed(top, total)
            for u in range(n_uly):
                last_out[where, u, 0:tokens, :] = result[u * tokens:(u + 1) * tokens]
                last_out[where, u, tokens:tokens + STAT, :] = turned(split, u * tokens, 0).astype(jnp.bfloat16)
        return finish

    def send_last(where, far, block=None):
        for d in (3, 2, 1, 0):
            src, dst = last_out.at[where, peers[d]], last_in.at[1 if far else 0, t]
            if d == 0 and not far:
                pltpu.make_async_copy(src, dst, last_own).start()
                continue
            place = {"uly": peers[d]} if block is None else {"seq": block, "uly": peers[d]}
            pltpu.make_async_remote_copy(
                src, dst, last_send, last_far.at[t] if far else last_own, device_id=place, device_id_type=MESH
            ).start()

    def join_last():
        landed(last_in.at[0], last_own)
        for pair in ((2, 3), (1, 0)):
            for d in pair:
                landed(last_in.at[1, peers[d]], last_far.at[peers[d]])
            for d in pair:
                u = peers[d]
                mine = level_of(last_in[0, u, tokens:tokens + STAT, :], 0)
                theirs = level_of(last_in[1, u, tokens:tokens + STAT, :], 0)
                top = jnp.maximum(mine, theirs)
                mine, theirs = jnp.exp2(mine - top), jnp.exp2(theirs - top)
                first = last_in[0, u, 0:tokens, :].astype(jnp.float32)
                second = last_in[1, u, 0:tokens, :].astype(jnp.float32)
                both = (first * mine + second * theirs) / (mine + theirs)
                back[:, columns(u, group - 1)] = both.astype(jnp.bfloat16)
        landed(back.at[:, 0:(group - 1) * n_uly * HEAD_DIM], back_sem)

    def merge(g, slot, a, lane=0):
        landed(part_in.at[slot, a], part_recv.at[slot, a])
        stats = part_in[slot, a, half:half + STAT, :]
        for chunk in range(2):
            level = level_of(stats, chunk)
            first = pl.multiple_of(a * half + chunk * HEAD_DIM, HEAD_DIM)
            cut = pl.ds(first, HEAD_DIM)
            top, total = own_stat[slot, 0, cut, :], own_stat[slot, 1, cut, :]
            new_top = jnp.maximum(top, level)
            mine, theirs = jnp.exp2(top - new_top), jnp.exp2(level - new_top)
            inverse = 1.0 / (total * mine + theirs)
            other = part_in[slot, a, chunk * HEAD_DIM:(chunk + 1) * HEAD_DIM, :].astype(jnp.float32)
            both = own[slot, cut, :] * (mine * inverse) + other * (theirs * inverse)
            att[lane, g, cut, :] = both.astype(jnp.bfloat16)

    def join(g, slot=None, lane=0):
        slot = g if slot is None else slot
        merge(g, slot, 1 - y, lane)
        give_back(g, (3, 2), lane)
        merge(g, slot, y, lane)
        give_back(g, (1, 0), lane)

    def each(first, count, body):
        def step(g, carry):
            body(g)
            return carry
        lax.fori_loop(first, count, step, 0)

    def add_up():
        for load in (past_load, *table_loads):
            load.wait()
        weights = [table_ref[0, slot_ref[p]] + table_ref[1, slot_ref[p]] for p in range(past.shape[0])]

        def sum_columns(uly):
            cols = pl.ds(pl.multiple_of(uly * (group * HEAD_DIM), HEAD_DIM), group * HEAD_DIM)
            mixed = weights[0] * past[0, :, cols].astype(jnp.float32)
            for p in range(1, past.shape[0]):
                mixed = mixed + weights[p] * past[p, :, cols].astype(jnp.float32)
            base_ref[:, cols] = mixed
        each(0, n_uly, sum_columns)

    def plane_sent():
        landed(given.at[:, :, 0:(n_uly - 1) * group * HEAD_DIM], plane_send)

    def line_sent(kind, block, first=0, count=group):
        landed(heads.at[kind, first:count, block], line_send.at[kind])

    def att_sent(first=0, count=group):
        if count > first:
            landed(att.at[0, first:count, 0:(n_uly - 1) * tokens, :], att_send.at[0])

    @pl.when(s == 0)
    def _():
        order = [(kind, g) for g in range(group) for kind in (K, V)]
        for kind, g in order[:2]:
            pass_on(kind, g, 0, 0, 1)

        @pl.when(ahead)
        def _():
            for kind, g in order[2:4]:
                pass_on(kind, g, 0, 0, 1)
        for i, (kind, g) in enumerate(order):
            scatter(kind, g, i if g == 0 else None)
        for g in range(group):
            scatter(Q, g)
        for i, (kind, g) in enumerate(order):
            if i < 2:
                @pl.when(behind)
                def _(i=i):
                    pass_on(*order[i + 2], 0, 0, 1)
            elif i + 2 < len(order):
                pass_on(*order[i + 2], 0, 0, 1)
            forward(kind, g, 0, 1, i if g == 0 else None)
        for i in range(2):
            gathered_piece(*order[i], 0, i)
        add_up()

        def work(g):
            gathered(Q, g)
            attend(g, 0, (), True, settle(g))
            give_back(g, (3, 2, 1, 0))
        each(0, group, work)
        plane_sent()
        for kind in (K, V):
            line_sent(kind, 0)
        att_sent()
        landed(back, back_sem)

    @pl.when(s == 1)
    def _():
        for g in range(group):
            for kind in (K, V, Q):
                scatter(kind, g)
        add_up()

        def begin(g, block):
            arrived(Q, g, block)
            attend(g, block, (1,), False, keep(block - 2))

        def end(g, block, finish):
            attend(g, block, (0,), False, finish, block - 2)

        def earliest(g):
            arrived(K, g, 0)

        def near(g):
            gathered(Q, g)
            attend(g, 1, (0,), True, settle(g))
            give_back(g, (3, 2, 1, 0))

        def work(g):
            for kind in (K, V):
                gathered(kind, g)
            begin(g, 2)
            earliest(g)
            end(g, 2, hand_over(g, 0))
            for a in (1 - y, y):
                partial(g, 0, a, 2, g)
            begin(g, 3)
            end(g, 3, hand_over(g, 1))
            stays = g < len(guests)
            for a in (1 - y, y):
                partial(g, 1, a, jnp.where(stays, 2, 3), jnp.where(stays, visit + g, g))
            near(g)
        each(0, group - 1, work)
        for kind in (K, V):
            gathered(kind, group - 1)
        begin(group - 1, 3)
        earliest(group - 1)
        end(group - 1, 3, hand_out(1))
        send_last(1, True, 3)
        begin(group - 1, 2)
        end(group - 1, 2, hand_out(0))
        send_last(0, True, 2)
        near(group - 1)
        plane_sent()
        landed(part_out, part_send)
        landed(last_out, last_send)
        att_sent()
        landed(back, back_sem)

    @pl.when(s == 2)
    def _():
        pass_on(Q, 0, 0, 2, 1)
        for kind in (K, V):
            pass_on(kind, hosts[0], 0, 2, 3)

        @pl.when(ahead)
        def _():
            for g in range(1, group):
                pass_on(Q, g, 0, 2, 1)
        order = [(Q, 0), (Q, 1)]
        for g in hosts:
            order += [(K, g), (V, g)] + ([(Q, g)] if g > 1 else [])
        order += [(Q, g) for g in range(2, hosts[0])]
        for kind, g in order:
            scatter(kind, g, g if kind == Q and g < 2 else None)
        for g in guests:
            for kind in (K, V):
                scatter(kind, g)
        for kind, g in order:
            to = 1 if kind == Q else 3
            if kind == Q and g > 0:
                @pl.when(behind)
                def _(g=g):
                    pass_on(Q, g, 0, 2, 1)
            elif kind != Q and g > hosts[0]:
                pass_on(kind, g, 0, 2, 3)
            if kind == Q and g == max(2, group - 1):
                relay(g)
            forward(kind, g, 2, to, g if kind == Q and g < 2 else None)
            if kind == Q and g < max(2, group - 1):
                relay(g)
        for g in range(2):
            gathered_piece(Q, g, 0, g)
        add_up()

        def near(g):
            attend(g, 2, (), True, keep(g))

        def own_guest(g):
            for kind in (K, V):
                gathered(kind, g)
            near(g)

        def receive(g):
            arrived(K, g, 3)
            attend(g, 3, (2,), True, keep(visit + g))

        attend(group - 1, 2, (), True, hand_out(0))
        send_last(0, False)
        each(hosts[0], group - 1, near)
        each(0, len(guests), own_guest)
        receive(0)
        join(0)
        join(0, visit, 1)
        for g in guests[1:]:
            join(g)
            receive(g)
            join(g, visit + g, 1)
        each(hosts[0], group - 1, join)
        join_last()
        plane_sent()
        line_sent(Q, 2)
        for kind in (K, V):
            line_sent(kind, 2, hosts[0])
        landed(heads.at[Q, :, 3], extra_send)
        landed(last_out.at[0, 0:n_uly - 1], last_send)
        landed(att.at[1, 0:len(guests)], att_send.at[1])
        att_sent(0, group - 1)

    @pl.when(s == 3)
    def _():
        for g in range(2):
            pass_on(Q, g, 0, 3, 2)

        @pl.when(ahead)
        def _():
            for g in range(2, group):
                pass_on(Q, g, 0, 3, 2)
        for g in range(group):
            scatter(Q, g, g if g < 2 else None)
        for g in (*guests, *hosts):
            for kind in (K, V):
                scatter(kind, g)
        for g in range(group):
            if g > 1:
                @pl.when(behind)
                def _(g=g):
                    pass_on(Q, g, 0, 3, 2)
            forward(Q, g, 3, 2, g if g < 2 else None)
        for g in guests:
            for kind in (K, V):
                pass_on(kind, g, 0, 3, 2)
                forward(kind, g, 3, 2)
        for g in range(2):
            gathered_piece(Q, g, 0, g)
        add_up()

        def near(g, finish=None):
            for kind in (K, V):
                gathered(kind, g)
            arrived(K, g, 2)
            attend(g, 3, (2,), True, keep(g) if finish is None else finish)
        each(hosts[0], group - 1, near)
        near(group - 1, hand_out(0))
        send_last(0, False)
        each(hosts[0], group - 1, join)
        join_last()
        plane_sent()
        line_sent(Q, 3)
        for kind in (K, V):
            line_sent(kind, 3, 0, len(guests))
        landed(last_out.at[0, 0:n_uly - 1], last_send)
        att_sent(hosts[0], group - 1)


def fused(queries, keys, values, past_outputs, dwa_slot, dwa_table):
    n_seq, n_uly = lax.axis_size("seq"), lax.axis_size("uly")
    tokens, features = queries.shape
    group = features // n_uly // HEAD_DIM
    rows = tokens * n_uly
    slots = group - 1 + max(1, group // 2)
    stored = past_outputs.shape[0]
    bf16, f32 = jnp.bfloat16, jnp.float32
    anywhere = pl.BlockSpec(memory_space=pltpu.HBM)
    attended, base = pl.pallas_call(
        functools.partial(fused_kernel, (n_seq, n_uly, group)),
        out_shape=(pltpu.VMEM((tokens, features), bf16), pltpu.VMEM((tokens, features), f32)),
        in_specs=[anywhere] * 6,
        out_specs=[pl.BlockSpec(memory_space=pltpu.VMEM)] * 2,
        scratch_shapes=[
            pltpu.SMEM(dwa_slot.shape, jnp.int32),
            pltpu.SMEM(dwa_table.shape, f32),
            pltpu.VMEM((3, tokens, features), bf16),
            pltpu.VMEM((stored, tokens, features), bf16),
            pltpu.VMEM((3, group, n_seq, rows, HEAD_DIM), bf16),
            pltpu.VMEM((slots, rows, HEAD_DIM), f32),
            pltpu.VMEM((slots, 2, rows, HEAD_DIM), f32),
            pltpu.VMEM((group - 1, 2, 2, rows // 2 + STAT, HEAD_DIM), bf16),
            pltpu.VMEM((slots, 2, rows // 2 + STAT, HEAD_DIM), bf16),
            pltpu.VMEM((2, group, rows, HEAD_DIM), bf16),
            pltpu.VMEM((2, n_uly, tokens + STAT, HEAD_DIM), bf16),
            pltpu.VMEM((2, n_uly, tokens + STAT, HEAD_DIM), bf16),
            pltpu.SemaphoreType.DMA,
            pltpu.SemaphoreType.DMA,
            pltpu.SemaphoreType.DMA((2,)),
            pltpu.SemaphoreType.DMA,
            pltpu.SemaphoreType.DMA((2, n_uly)),
            pltpu.SemaphoreType.DMA((2, n_uly)),
            pltpu.SemaphoreType.DMA((3, group)),
            pltpu.SemaphoreType.DMA((3,)),
            pltpu.SemaphoreType.DMA,
            pltpu.SemaphoreType.DMA((3, group)),
            pltpu.SemaphoreType.DMA,
            pltpu.SemaphoreType.DMA((slots, 2)),
            pltpu.SemaphoreType.DMA((2,)),
            pltpu.SemaphoreType.DMA,
            pltpu.SemaphoreType.DMA,
            pltpu.SemaphoreType.DMA,
            pltpu.SemaphoreType.DMA((n_uly,)),
        ],
        compiler_params=pltpu.CompilerParams(
            collective_id=0, has_side_effects=True, vmem_limit_bytes=32 * 1024 * 1024
        ),
    )(*(pltpu.with_memory_space_constraint(x, pltpu.HBM) for x in (dwa_slot, dwa_table, queries, keys, values, past_outputs)))
    return (base + attended.astype(f32)).astype(bf16)


def solution(mesh):
    def body(queries, *rest):
        heads_here = queries.shape[1] // HEAD_DIM // mesh.shape["uly"]
        fits = mesh.shape["seq"] == SPAN and mesh.shape["uly"] == PLANE and heads_here >= 2
        return (fused if fits else shards)(queries, *rest)

    return jax.shard_map(
        body,
        mesh=mesh,
        in_specs=(
            P(("rep", "seq", "uly"), None),
            P(("rep", "seq", "uly"), None),
            P(("rep", "seq", "uly"), None),
            P(None, ("rep", "seq", "uly"), None),
            P(),
            P(),
        ),
        out_specs=P(("rep", "seq", "uly"), None),
        check_vma=False,
    )
```

```python
import functools
import math

import jax
import jax.numpy as jnp
from jax import lax
from jax.experimental import pallas as pl
from jax.experimental.pallas import tpu as pltpu
from jax.sharding import PartitionSpec as P

HEAD_DIM = 128
SPAN = 4
PLANE = 4
STAT = 8
MESH = pl.DeviceIdType.MESH
Q, K, V = 0, 1, 2


def from_behind(block, axis, distance):
    devices = range(lax.axis_size(axis))
    route = [(i - distance, i) for i in devices if i - distance in devices]
    return lax.ppermute(block, axis, route)


def block_update(state, query_heads, key_heads, value_heads, allowed):
    running, total, accumulated = state
    scores = jnp.einsum("qhd,khd->hqk", query_heads, key_heads, preferred_element_type=jnp.float32)
    scores = scores * (1.0 / HEAD_DIM**0.5)
    scores = jnp.where(allowed, scores, -jnp.inf)
    new_max = jnp.maximum(running, jnp.max(scores, axis=2))
    factor = jnp.exp(running - new_max)
    prob = jnp.exp(scores - new_max[:, :, None])
    total = total * factor + jnp.sum(prob, axis=2)
    weights = prob.astype(jnp.bfloat16)
    update = jnp.einsum("hqk,khd->qhd", weights, value_heads, preferred_element_type=jnp.float32)
    accumulated = accumulated * jnp.transpose(factor)[:, :, None] + update
    return (new_max, total, accumulated)


def shards(queries, keys, values, past_outputs, dwa_slot, dwa_table):
    n_uly = lax.axis_size("uly")
    n_seq = lax.axis_size("seq")
    span_size = min(4, n_seq)
    features = queries.shape[1]
    local_heads = features // n_uly // HEAD_DIM
    query_rows, key_rows, value_rows = (
        lax.all_to_all(queries, "uly", split_axis=1, concat_axis=0, tiled=True),
        lax.all_to_all(keys, "uly", split_axis=1, concat_axis=0, tiled=True),
        lax.all_to_all(values, "uly", split_axis=1, concat_axis=0, tiled=True),
    )
    row_count = query_rows.shape[0]
    split_shape = (row_count, local_heads, HEAD_DIM)
    query_heads = query_rows.reshape(split_shape)
    table_index = jnp.arange(dwa_table.shape[1])
    onehot = (dwa_slot[:, None] == table_index[None, :]).astype(jnp.float32)
    coefs = jnp.dot(onehot, jnp.transpose(dwa_table), precision=lax.Precision.HIGHEST)
    layer_in = jnp.zeros(queries.shape, jnp.float32)
    extra = jnp.zeros(queries.shape, jnp.float32)
    for index in range(past_outputs.shape[0]):
        stored = past_outputs[index].astype(jnp.float32)
        layer_in = layer_in + coefs[index, 0] * stored
        extra = extra + coefs[index, 1] * stored
    running = jnp.full((local_heads, row_count), -jnp.inf, jnp.float32)
    total = jnp.zeros((local_heads, row_count), jnp.float32)
    accumulated = jnp.zeros(split_shape, jnp.float32)
    state = (running, total, accumulated)
    causal = (jnp.arange(row_count)[:, None] >= jnp.arange(row_count)[None, :])[None, :, :]
    state = block_update(
        state, query_heads, key_rows.reshape(split_shape), value_rows.reshape(split_shape), causal
    )
    position = lax.axis_index("seq")
    current = (key_rows, value_rows)
    for offset in range(1, span_size):
        current = from_behind((current[0], current[1]), "seq", 1)
        far_keys = current[0].reshape(split_shape)
        far_values = current[1].reshape(split_shape)

        def take_block(carry, far_keys=far_keys, far_values=far_values):
            return block_update(carry, query_heads, far_keys, far_values, True)

        def keep_block(carry):
            return carry

        state = lax.cond(position >= offset, take_block, keep_block, state)
    running, total, accumulated = state
    attended = accumulated / jnp.transpose(total)[:, :, None]
    attended = attended.astype(jnp.bfloat16).reshape(row_count, local_heads * HEAD_DIM)
    returned = lax.all_to_all(attended, "uly", split_axis=0, concat_axis=1, tiled=True)
    hidden = layer_in + returned.astype(jnp.float32)
    return (hidden + extra).astype(jnp.bfloat16)


def fused_kernel(
    shape,
    slot_hbm, table_hbm, q_hbm, k_hbm, v_hbm, past_hbm, back, base_ref,
    slot_ref, table_ref, given, past, heads, own, own_stat, part_out, part_in, att, last_out, last_in,
    load_sem, past_sem, table_sem, plane_send, piece_sem, relay_sem, whole_sem, line_send, extra_send, line_recv, early_recv,
    part_send, part_recv, att_send, back_sem, last_send, last_own, last_far,
):
    n_seq, n_uly, group = shape
    tokens = given.shape[1]
    rows = n_uly * tokens
    half = rows // 2
    scale = math.log2(math.e) / HEAD_DIM**0.5
    s, t = lax.axis_index("seq"), lax.axis_index("uly")
    y, x = t // 2, t % 2
    ahead = lax.axis_index("rep") % 2 == 1
    behind = jnp.logical_not(ahead)
    peers = (t, 2 * y + 1 - x, 2 * (1 - y) + x, 3 - t)
    guests = range(max(1, group // 2))
    hosts = range(len(guests), group)
    visit = group - 1
    lanes = {(Q, 2): 0, (Q, 3): 1, (K, 0): 2, (V, 0): 2, (K, 2): 2, (V, 2): 2, (K, 3): 2, (V, 3): 2}

    loads = [
        pltpu.make_async_copy(src, given.at[i], load_sem) for i, src in enumerate((q_hbm, k_hbm, v_hbm))
    ]
    table_loads = [
        pltpu.make_async_copy(src, dst, table_sem.at[i])
        for i, (src, dst) in enumerate(((slot_hbm, slot_ref), (table_hbm, table_ref)))
    ]
    past_load = pltpu.make_async_copy(past_hbm, past, past_sem)
    for load in (*loads, past_load, *table_loads):
        load.start()

    def landed(ref, sem):
        pltpu.make_async_copy(ref, ref, sem).wait()

    barrier = pltpu.get_barrier_semaphore()
    for d in (1, 2, 3):
        pl.semaphore_signal(barrier, inc=1, device_id={"uly": peers[d]}, device_id_type=MESH)
    neighbours = {0: (1,), 1: (0, 2, 3), 2: (1, 3), 3: (1, 2)}
    for place, others in neighbours.items():
        @pl.when(s == place)
        def _(place=place, others=others):
            for other in others:
                pl.semaphore_signal(barrier, inc=1, device_id={"seq": other}, device_id_type=MESH)
            if place == 3:
                for d in (1, 2, 3):
                    pl.semaphore_signal(barrier, inc=1, device_id={"seq": 2, "uly": peers[d]}, device_id_type=MESH)
            pl.semaphore_wait(barrier, 3 + len(others) + (3 if place == 2 else 0))
    landed(given, load_sem)

    def columns(uly, g):
        return pl.ds(pl.multiple_of((uly * group + g) * HEAD_DIM, HEAD_DIM), HEAD_DIM)

    def row_range(uly):
        return pl.ds(pl.multiple_of(uly * tokens, tokens), tokens)

    def scatter(kind, g, pieces=None):
        for d in (1, 2, 3, 0):
            src = given.at[kind, :, columns(peers[d], g)]
            dst = heads.at[kind, g, s, row_range(t), :]
            sem = whole_sem.at[kind, g] if pieces is None else piece_sem.at[pieces, d]
            if d == 0:
                pltpu.make_async_copy(src, dst, sem).start()
            else:
                pltpu.make_async_remote_copy(
                    src, dst, plane_send, sem, device_id={"uly": peers[d]}, device_id_type=MESH
                ).start()

    def gathered(kind, g):
        landed(heads.at[kind, g, s], whole_sem.at[kind, g])

    def gathered_piece(kind, g, d, pieces):
        landed(heads.at[kind, g, s, row_range(peers[d]), :], piece_sem.at[pieces, d])

    def arrived(kind, g, block):
        ref = heads.at[Q, g, block] if kind == Q else heads.at[K:V + 1, g, block]
        landed(ref, line_recv.at[lanes[kind, block], g])

    def pass_on(kind, g, d, block, to):
        dst = heads.at[kind, g, block, row_range(peers[d]), :]
        src = given.at[kind, :, columns(t, g)] if d == 0 else dst
        piecewise = kind == Q and block == 3 and g < 2
        if block == 1:
            sem = early_recv.at[1]
        else:
            sem = relay_sem.at[g, d] if piecewise else line_recv.at[lanes[kind, block], g]
        pltpu.make_async_remote_copy(
            src, dst, line_send.at[kind], sem,
            device_id={"seq": to}, device_id_type=MESH,
        ).start()

    def forward(kind, g, block, to, pieces=None):
        if pieces is None:
            gathered(kind, g)
        for d in (1, 2, 3):
            if pieces is not None:
                gathered_piece(kind, g, d, pieces)
            pass_on(kind, g, d, block, to)

    def relay(g):
        parts = [heads.at[Q, g, 3]]
        if g < 2:
            parts = [heads.at[Q, g, 3, row_range(peers[d]), :] for d in range(n_uly)]
        for d, ref in enumerate(parts):
            landed(ref, relay_sem.at[g, d] if g < 2 else line_recv.at[lanes[Q, 3], g])
            pltpu.make_async_remote_copy(
                ref, ref, extra_send, line_recv.at[lanes[Q, 3], g], device_id={"seq": 1}, device_id_type=MESH
            ).start()

    def partial(g, where, a, to, slot):
        pltpu.make_async_remote_copy(
            part_out.at[g, where, a], part_in.at[slot, a], part_send, part_recv.at[slot, a],
            device_id={"seq": to}, device_id_type=MESH,
        ).start()

    def give_back(g, ds, lane=0):
        for d in ds:
            src = att.at[lane, g, row_range(peers[d]), :]
            dst = back.at[:, columns(t, g)]
            if lane == 0 and d == 0:
                pltpu.make_async_copy(src, dst, back_sem).start()
                continue
            where = {"uly": peers[d]} if lane == 0 else {"seq": n_seq - 1, "uly": peers[d]}
            pltpu.make_async_remote_copy(
                src, dst, att_send.at[lane], back_sem, device_id=where, device_id_type=MESH
            ).start()

    def attend(g, block, full, diagonal, finish, resume=None):
        query = heads[Q, g, block]
        acc_shape = (rows, HEAD_DIM)
        top = total = acc = None
        if resume is not None:
            top, total, acc = own_stat[resume, 0], own_stat[resume, 1], own[resume]
        for j in (*full, block) if diagonal else full:
            key = heads[K, g, j]
            value = heads[V, g, j]
            scores = lax.dot_general(query, key, (((1,), (1,)), ((), ())), preferred_element_type=jnp.float32)
            scores = scores * scale
            if j == block:
                query_at = lax.broadcasted_iota(jnp.int32, scores.shape, 0)
                key_at = lax.broadcasted_iota(jnp.int32, scores.shape, 1)
                scores = jnp.where(key_at <= query_at, scores, -jnp.inf)
            peak = jnp.broadcast_to(jnp.max(scores, axis=1, keepdims=True), acc_shape)
            new_top = peak if top is None else jnp.maximum(top, peak)
            prob = jnp.exp2(scores - jnp.concatenate([new_top] * (rows // HEAD_DIM), axis=1))
            sums = jnp.broadcast_to(jnp.sum(prob, axis=1, keepdims=True), acc_shape)
            update = jnp.dot(prob.astype(jnp.bfloat16), value, preferred_element_type=jnp.float32)
            if top is None:
                total, acc = sums, update
            else:
                factor = jnp.exp2(top - new_top)
                total = total * factor + sums
                acc = acc * factor + update
            top = new_top
        finish(top, total, acc)

    def settle(g, lane=0):
        def finish(top, total, acc):
            att[lane, g] = (acc / total).astype(jnp.bfloat16)
        return finish

    def keep(slot):
        def finish(top, total, acc):
            own[slot] = acc
            own_stat[slot, 0] = top
            own_stat[slot, 1] = total
        return finish

    def selector(shape, dim, chunk):
        place = lax.broadcasted_iota(jnp.int32, shape, dim) - 3 * chunk
        other = lax.broadcasted_iota(jnp.int32, shape, 1 - dim)
        return place, other

    def packed(top, total):
        level = top + jnp.log2(total)
        high = level.astype(jnp.bfloat16).astype(jnp.float32)
        middle = (level - high).astype(jnp.bfloat16).astype(jnp.float32)
        low = level - high - middle
        lane = lax.broadcasted_iota(jnp.int32, (rows, HEAD_DIM), 1)
        split = jnp.where(lane == 0, high, jnp.where(lane == 1, middle, jnp.where(lane == 2, low, 0.0)))
        return split.astype(jnp.bfloat16)

    def turned(split, first, chunk):
        place, other = selector((STAT, HEAD_DIM), 0, chunk)
        pick = jnp.where((place == other) & (other < 3), 1.0, 0.0).astype(jnp.bfloat16)
        return lax.dot_general(
            pick, split[first:first + HEAD_DIM], (((1,), (1,)), ((), ())), preferred_element_type=jnp.float32
        )

    def level_of(stats, chunk):
        place, _ = selector((STAT, HEAD_DIM), 0, chunk)
        ones = jnp.where((place >= 0) & (place < 3), 1.0, 0.0).astype(jnp.bfloat16)
        return lax.dot_general(stats, ones, (((0,), (0,)), ((), ())), preferred_element_type=jnp.float32)

    def hand_over(g, where):
        def finish(top, total, acc):
            result = (acc / total).astype(jnp.bfloat16)
            split = packed(top, total)
            for a in range(2):
                part_out[g, where, a, 0:half, :] = result[a * half:(a + 1) * half]
                stats = turned(split, a * half, 0) + turned(split, a * half + HEAD_DIM, 1)
                part_out[g, where, a, half:half + STAT, :] = stats.astype(jnp.bfloat16)
        return finish

    def hand_out(where):
        def finish(top, total, acc):
            result = (acc / total).astype(jnp.bfloat16)
            split = packed(top, total)
            for u in range(n_uly):
                last_out[where, u, 0:tokens, :] = result[u * tokens:(u + 1) * tokens]
                last_out[where, u, tokens:tokens + STAT, :] = turned(split, u * tokens, 0).astype(jnp.bfloat16)
        return finish

    def send_last(where, far, block=None):
        for d in (3, 2, 1, 0):
            src, dst = last_out.at[where, peers[d]], last_in.at[1 if far else 0, t]
            if d == 0 and not far:
                pltpu.make_async_copy(src, dst, last_own).start()
                continue
            place = {"uly": peers[d]} if block is None else {"seq": block, "uly": peers[d]}
            pltpu.make_async_remote_copy(
                src, dst, last_send, last_far.at[t] if far else last_own, device_id=place, device_id_type=MESH
            ).start()

    def join_last():
        landed(last_in.at[0], last_own)
        for pair in ((2, 3), (1, 0)):
            for d in pair:
                landed(last_in.at[1, peers[d]], last_far.at[peers[d]])
            for d in pair:
                u = peers[d]
                mine = level_of(last_in[0, u, tokens:tokens + STAT, :], 0)
                theirs = level_of(last_in[1, u, tokens:tokens + STAT, :], 0)
                top = jnp.maximum(mine, theirs)
                mine, theirs = jnp.exp2(mine - top), jnp.exp2(theirs - top)
                first = last_in[0, u, 0:tokens, :].astype(jnp.float32)
                second = last_in[1, u, 0:tokens, :].astype(jnp.float32)
                both = (first * mine + second * theirs) / (mine + theirs)
                back[:, columns(u, group - 1)] = both.astype(jnp.bfloat16)
        landed(back.at[:, 0:(group - 1) * n_uly * HEAD_DIM], back_sem)

    def merge(g, slot, a, lane=0):
        landed(part_in.at[slot, a], part_recv.at[slot, a])
        stats = part_in[slot, a, half:half + STAT, :]
        for chunk in range(2):
            level = level_of(stats, chunk)
            first = pl.multiple_of(a * half + chunk * HEAD_DIM, HEAD_DIM)
            cut = pl.ds(first, HEAD_DIM)
            top, total = own_stat[slot, 0, cut, :], own_stat[slot, 1, cut, :]
            new_top = jnp.maximum(top, level)
            mine, theirs = jnp.exp2(top - new_top), jnp.exp2(level - new_top)
            inverse = 1.0 / (total * mine + theirs)
            other = part_in[slot, a, chunk * HEAD_DIM:(chunk + 1) * HEAD_DIM, :].astype(jnp.float32)
            both = own[slot, cut, :] * (mine * inverse) + other * (theirs * inverse)
            att[lane, g, cut, :] = both.astype(jnp.bfloat16)

    def join(g, slot=None, lane=0):
        slot = g if slot is None else slot
        merge(g, slot, 1 - y, lane)
        give_back(g, (3, 2), lane)
        merge(g, slot, y, lane)
        give_back(g, (1, 0), lane)

    def each(first, count, body):
        def step(g, carry):
            body(g)
            return carry
        lax.fori_loop(first, count, step, 0)

    def add_up():
        for load in (past_load, *table_loads):
            load.wait()
        weights = [table_ref[0, slot_ref[p]] + table_ref[1, slot_ref[p]] for p in range(past.shape[0])]

        def sum_columns(uly):
            cols = pl.ds(pl.multiple_of(uly * (group * HEAD_DIM), HEAD_DIM), group * HEAD_DIM)
            mixed = weights[0] * past[0, :, cols].astype(jnp.float32)
            for p in range(1, past.shape[0]):
                mixed = mixed + weights[p] * past[p, :, cols].astype(jnp.float32)
            base_ref[:, cols] = mixed
        each(0, n_uly, sum_columns)

    def plane_sent():
        landed(given.at[:, :, 0:(n_uly - 1) * group * HEAD_DIM], plane_send)

    def line_sent(kind, block, first=0, count=group):
        landed(heads.at[kind, first:count, block], line_send.at[kind])

    def att_sent(first=0, count=group):
        if count > first:
            landed(att.at[0, first:count, 0:(n_uly - 1) * tokens, :], att_send.at[0])

    @pl.when(s == 0)
    def _():
        order = [(kind, g) for g in range(group) for kind in (K, V)]
        for kind, g in order[:2]:
            pass_on(kind, g, 0, 0, 1)

        @pl.when(ahead)
        def _():
            for kind, g in order[2:4]:
                pass_on(kind, g, 0, 0, 1)
        for i, (kind, g) in enumerate(order):
            scatter(kind, g, i if g == 0 else None)
        for g in range(group):
            scatter(Q, g)
        for i, (kind, g) in enumerate(order):
            if i < 2:
                @pl.when(behind)
                def _(i=i):
                    pass_on(*order[i + 2], 0, 0, 1)
            elif i + 2 < len(order):
                pass_on(*order[i + 2], 0, 0, 1)
            forward(kind, g, 0, 1, i if g == 0 else None)
        for i in range(2):
            gathered_piece(*order[i], 0, i)
        add_up()

        def work(g):
            gathered(Q, g)
            attend(g, 0, (), True, settle(g))
            give_back(g, (3, 2, 1, 0))
        each(0, group, work)
        plane_sent()
        for kind in (K, V):
            line_sent(kind, 0)
        att_sent()
        landed(back, back_sem)

    @pl.when(s == 1)
    def _():
        for kind in (K, V):
            pass_on(kind, 0, 0, 1, 2)
        for i, kind in enumerate((K, V)):
            scatter(kind, 0, i)
        for kind in (K, V):
            scatter(kind, 1)
        scatter(Q, 1)
        scatter(Q, 0)
        for g in range(2, group):
            for kind in (K, V, Q):
                scatter(kind, g)
        for i, kind in enumerate((K, V)):
            forward(kind, 0, 1, 2, i)
            gathered_piece(kind, 0, 0, i)
        add_up()

        def begin(g, block):
            arrived(Q, g, block)
            attend(g, block, (1,), False, keep(block - 2))

        def end(g, block, finish):
            attend(g, block, (0,), False, finish, block - 2)

        def earliest(g):
            arrived(K, g, 0)

        def near(g):
            gathered(Q, g)
            attend(g, 1, (0,), True, settle(g))
            give_back(g, (3, 2, 1, 0))

        def work(g):
            for kind in (K, V):
                gathered(kind, g)
            begin(g, 2)
            earliest(g)
            end(g, 2, hand_over(g, 0))
            for a in (1 - y, y):
                partial(g, 0, a, 2, g)
            begin(g, 3)
            end(g, 3, hand_over(g, 1))
            stays = g < len(guests)
            for a in (1 - y, y):
                partial(g, 1, a, jnp.where(stays, 2, 3), jnp.where(stays, visit + g, g))
            near(g)
        earliest(0)
        for kind in (K, V):
            ref = heads.at[kind, 0, 0]
            pltpu.make_async_remote_copy(
                ref, ref, line_send.at[kind], early_recv.at[0], device_id={"seq": 2}, device_id_type=MESH
            ).start()
        near(0)
        each(1, group - 1, work)
        for kind in (K, V):
            gathered(kind, group - 1)
        begin(group - 1, 3)
        earliest(group - 1)
        end(group - 1, 3, hand_out(1))
        send_last(1, True, 3)
        begin(group - 1, 2)
        end(group - 1, 2, hand_out(0))
        send_last(0, True, 2)
        near(group - 1)
        plane_sent()
        landed(part_out.at[1:], part_send)
        for kind in (K, V):
            landed(heads.at[kind, 0, 0:2], line_send.at[kind])
        landed(last_out, last_send)
        att_sent()
        landed(back, back_sem)

    @pl.when(s == 2)
    def _():
        for kind in (K, V):
            pass_on(kind, hosts[0], 0, 2, 3)
        pass_on(Q, 1, 0, 2, 1)

        @pl.when(ahead)
        def _():
            for g in range(2, group):
                pass_on(Q, g, 0, 2, 1)
        order = [(Q, 1)]
        for g in hosts:
            order += [(K, g), (V, g)] + ([(Q, g)] if g > 1 else [])
        order += [(Q, g) for g in range(2, hosts[0])]
        for kind, g in order:
            scatter(kind, g, g if kind == Q and g < 2 else None)
        scatter(Q, 0)
        for g in guests:
            for kind in (K, V):
                scatter(kind, g)
        for kind, g in order:
            to = 1 if kind == Q else 3
            if kind == Q and g > 1:
                @pl.when(behind)
                def _(g=g):
                    pass_on(Q, g, 0, 2, 1)
            elif kind != Q and g > hosts[0]:
                pass_on(kind, g, 0, 2, 3)
            if kind == Q and g == max(2, group - 1):
                relay(g)
            forward(kind, g, 2, to, g if kind == Q and g < 2 else None)
            if kind == Q and g < max(2, group - 1):
                relay(g)
        gathered_piece(Q, 1, 0, 1)
        add_up()

        def near(g):
            attend(g, 2, (), True, keep(g))

        def own_guest(g):
            for kind in (K, V):
                gathered(kind, g)

        attend(group - 1, 2, (), True, hand_out(0))
        send_last(0, False)
        each(hosts[0], group - 1, near)
        gathered(Q, 0)
        own_guest(0)
        for i in (1, 0):
            landed(heads.at[K:V + 1, 0, i], early_recv.at[i])
        attend(0, 2, (0, 1), True, settle(0))
        give_back(0, (3, 2, 1, 0))
        for d in range(n_uly):
            landed(heads.at[Q, 0, 3, row_range(peers[d]), :], relay_sem.at[0, d])
        arrived(K, 0, 3)
        attend(0, 3, (0, 1, 2), True, settle(0, 1))
        give_back(0, (3, 2, 1, 0), 1)
        for g in guests[1:]:
            own_guest(g)
            near(g)
            join(g)
            arrived(K, g, 3)
            attend(g, 3, (2,), True, keep(visit + g))
            join(g, visit + g, 1)
        each(hosts[0], group - 1, join)
        join_last()
        plane_sent()
        line_sent(Q, 2, 1)
        for kind in (K, V):
            line_sent(kind, 2, hosts[0])
        landed(heads.at[Q, 1:, 3], extra_send)
        landed(last_out.at[0, 0:n_uly - 1], last_send)
        landed(att.at[1, 0:len(guests)], att_send.at[1])
        att_sent(0, group - 1)

    @pl.when(s == 3)
    def _():
        order = [(Q, g) for g in (*range(1, group), 0)] + [(kind, g) for g in guests for kind in (K, V)]
        pass_on(Q, 1, 0, 3, 2)

        @pl.when(ahead)
        def _():
            for g in range(2, group):
                pass_on(Q, g, 0, 3, 2)
        for kind, g in order:
            scatter(kind, g, g if kind == Q and g < 2 else None)
        for g in hosts:
            for kind in (K, V):
                scatter(kind, g)
        for kind, g in order:
            if kind != Q or g == 0:
                pass_on(kind, g, 0, 3, 2)
            elif g > 1:
                @pl.when(behind)
                def _(g=g):
                    pass_on(Q, g, 0, 3, 2)
            forward(kind, g, 3, 2, g if kind == Q and g < 2 else None)
        for g in range(2):
            gathered_piece(Q, g, 0, g)
        add_up()

        def near(g, finish=None):
            for kind in (K, V):
                gathered(kind, g)
            arrived(K, g, 2)
            attend(g, 3, (2,), True, keep(g) if finish is None else finish)
        each(hosts[0], group - 1, near)
        near(group - 1, hand_out(0))
        send_last(0, False)
        each(hosts[0], group - 1, join)
        join_last()
        plane_sent()
        line_sent(Q, 3)
        for kind in (K, V):
            line_sent(kind, 3, 0, len(guests))
        landed(last_out.at[0, 0:n_uly - 1], last_send)
        att_sent(hosts[0], group - 1)


def fused(queries, keys, values, past_outputs, dwa_slot, dwa_table):
    n_seq, n_uly = lax.axis_size("seq"), lax.axis_size("uly")
    tokens, features = queries.shape
    group = features // n_uly // HEAD_DIM
    rows = tokens * n_uly
    slots = group - 1 + max(1, group // 2)
    stored = past_outputs.shape[0]
    bf16, f32 = jnp.bfloat16, jnp.float32
    anywhere = pl.BlockSpec(memory_space=pltpu.HBM)
    attended, base = pl.pallas_call(
        functools.partial(fused_kernel, (n_seq, n_uly, group)),
        out_shape=(pltpu.VMEM((tokens, features), bf16), pltpu.VMEM((tokens, features), f32)),
        in_specs=[anywhere] * 6,
        out_specs=[pl.BlockSpec(memory_space=pltpu.VMEM)] * 2,
        scratch_shapes=[
            pltpu.SMEM(dwa_slot.shape, jnp.int32),
            pltpu.SMEM(dwa_table.shape, f32),
            pltpu.VMEM((3, tokens, features), bf16),
            pltpu.VMEM((stored, tokens, features), bf16),
            pltpu.VMEM((3, group, n_seq, rows, HEAD_DIM), bf16),
            pltpu.VMEM((slots, rows, HEAD_DIM), f32),
            pltpu.VMEM((slots, 2, rows, HEAD_DIM), f32),
            pltpu.VMEM((group - 1, 2, 2, rows // 2 + STAT, HEAD_DIM), bf16),
            pltpu.VMEM((slots, 2, rows // 2 + STAT, HEAD_DIM), bf16),
            pltpu.VMEM((2, group, rows, HEAD_DIM), bf16),
            pltpu.VMEM((2, n_uly, tokens + STAT, HEAD_DIM), bf16),
            pltpu.VMEM((2, n_uly, tokens + STAT, HEAD_DIM), bf16),
            pltpu.SemaphoreType.DMA,
            pltpu.SemaphoreType.DMA,
            pltpu.SemaphoreType.DMA((2,)),
            pltpu.SemaphoreType.DMA,
            pltpu.SemaphoreType.DMA((2, n_uly)),
            pltpu.SemaphoreType.DMA((2, n_uly)),
            pltpu.SemaphoreType.DMA((3, group)),
            pltpu.SemaphoreType.DMA((3,)),
            pltpu.SemaphoreType.DMA,
            pltpu.SemaphoreType.DMA((3, group)),
            pltpu.SemaphoreType.DMA((2,)),
            pltpu.SemaphoreType.DMA,
            pltpu.SemaphoreType.DMA((slots, 2)),
            pltpu.SemaphoreType.DMA((2,)),
            pltpu.SemaphoreType.DMA,
            pltpu.SemaphoreType.DMA,
            pltpu.SemaphoreType.DMA,
            pltpu.SemaphoreType.DMA((n_uly,)),
        ],
        compiler_params=pltpu.CompilerParams(
            collective_id=0, has_side_effects=True, vmem_limit_bytes=32 * 1024 * 1024
        ),
    )(*(pltpu.with_memory_space_constraint(x, pltpu.HBM) for x in (dwa_slot, dwa_table, queries, keys, values, past_outputs)))
    return (base + attended.astype(f32)).astype(bf16)


def solution(mesh):
    def body(queries, *rest):
        heads_here = queries.shape[1] // HEAD_DIM // mesh.shape["uly"]
        fits = mesh.shape["seq"] == SPAN and mesh.shape["uly"] == PLANE and heads_here >= 2
        return (fused if fits else shards)(queries, *rest)

    return jax.shard_map(
        body,
        mesh=mesh,
        in_specs=(
            P(("rep", "seq", "uly"), None),
            P(("rep", "seq", "uly"), None),
            P(("rep", "seq", "uly"), None),
            P(None, ("rep", "seq", "uly"), None),
            P(),
            P(),
        ),
        out_specs=P(("rep", "seq", "uly"), None),
        check_vma=False,
    )
```

```python
import functools
import math

import jax
import jax.numpy as jnp
from jax import lax
from jax.experimental import pallas as pl
from jax.experimental.pallas import tpu as pltpu
from jax.sharding import PartitionSpec as P

HEAD_DIM = 128
SPAN = 4
PLANE = 4
STAT = 8
MESH = pl.DeviceIdType.MESH
Q, K, V = 0, 1, 2


def from_behind(block, axis, distance):
    devices = range(lax.axis_size(axis))
    route = [(i - distance, i) for i in devices if i - distance in devices]
    return lax.ppermute(block, axis, route)


def block_update(state, query_heads, key_heads, value_heads, allowed):
    running, total, accumulated = state
    scores = jnp.einsum("qhd,khd->hqk", query_heads, key_heads, preferred_element_type=jnp.float32)
    scores = scores * (1.0 / HEAD_DIM**0.5)
    scores = jnp.where(allowed, scores, -jnp.inf)
    new_max = jnp.maximum(running, jnp.max(scores, axis=2))
    factor = jnp.exp(running - new_max)
    prob = jnp.exp(scores - new_max[:, :, None])
    total = total * factor + jnp.sum(prob, axis=2)
    weights = prob.astype(jnp.bfloat16)
    update = jnp.einsum("hqk,khd->qhd", weights, value_heads, preferred_element_type=jnp.float32)
    accumulated = accumulated * jnp.transpose(factor)[:, :, None] + update
    return (new_max, total, accumulated)


def shards(queries, keys, values, past_outputs, dwa_slot, dwa_table):
    n_uly = lax.axis_size("uly")
    n_seq = lax.axis_size("seq")
    span_size = min(4, n_seq)
    features = queries.shape[1]
    local_heads = features // n_uly // HEAD_DIM
    query_rows, key_rows, value_rows = (
        lax.all_to_all(queries, "uly", split_axis=1, concat_axis=0, tiled=True),
        lax.all_to_all(keys, "uly", split_axis=1, concat_axis=0, tiled=True),
        lax.all_to_all(values, "uly", split_axis=1, concat_axis=0, tiled=True),
    )
    row_count = query_rows.shape[0]
    split_shape = (row_count, local_heads, HEAD_DIM)
    query_heads = query_rows.reshape(split_shape)
    table_index = jnp.arange(dwa_table.shape[1])
    onehot = (dwa_slot[:, None] == table_index[None, :]).astype(jnp.float32)
    coefs = jnp.dot(onehot, jnp.transpose(dwa_table), precision=lax.Precision.HIGHEST)
    layer_in = jnp.zeros(queries.shape, jnp.float32)
    extra = jnp.zeros(queries.shape, jnp.float32)
    for index in range(past_outputs.shape[0]):
        stored = past_outputs[index].astype(jnp.float32)
        layer_in = layer_in + coefs[index, 0] * stored
        extra = extra + coefs[index, 1] * stored
    running = jnp.full((local_heads, row_count), -jnp.inf, jnp.float32)
    total = jnp.zeros((local_heads, row_count), jnp.float32)
    accumulated = jnp.zeros(split_shape, jnp.float32)
    state = (running, total, accumulated)
    causal = (jnp.arange(row_count)[:, None] >= jnp.arange(row_count)[None, :])[None, :, :]
    state = block_update(
        state, query_heads, key_rows.reshape(split_shape), value_rows.reshape(split_shape), causal
    )
    position = lax.axis_index("seq")
    current = (key_rows, value_rows)
    for offset in range(1, span_size):
        current = from_behind((current[0], current[1]), "seq", 1)
        far_keys = current[0].reshape(split_shape)
        far_values = current[1].reshape(split_shape)

        def take_block(carry, far_keys=far_keys, far_values=far_values):
            return block_update(carry, query_heads, far_keys, far_values, True)

        def keep_block(carry):
            return carry

        state = lax.cond(position >= offset, take_block, keep_block, state)
    running, total, accumulated = state
    attended = accumulated / jnp.transpose(total)[:, :, None]
    attended = attended.astype(jnp.bfloat16).reshape(row_count, local_heads * HEAD_DIM)
    returned = lax.all_to_all(attended, "uly", split_axis=0, concat_axis=1, tiled=True)
    hidden = layer_in + returned.astype(jnp.float32)
    return (hidden + extra).astype(jnp.bfloat16)


def fused_kernel(
    shape,
    slot_hbm, table_hbm, q_hbm, k_hbm, v_hbm, past_hbm, back, base_ref,
    slot_ref, table_ref, given, past, heads, own, own_stat, part_out, part_in, att, last_out, last_in,
    load_sem, past_sem, table_sem, plane_send, piece_sem, relay_sem, whole_sem, line_send, extra_send, line_recv, early_recv,
    part_send, part_recv, att_send, back_sem, last_send, last_own, last_far,
):
    n_seq, n_uly, group = shape
    tokens = given.shape[1]
    rows = n_uly * tokens
    half = rows // 2
    scale = math.log2(math.e) / HEAD_DIM**0.5
    s, t = lax.axis_index("seq"), lax.axis_index("uly")
    y, x = t // 2, t % 2
    ahead = lax.axis_index("rep") % 2 == 1
    behind = jnp.logical_not(ahead)
    peers = (t, 2 * y + 1 - x, 2 * (1 - y) + x, 3 - t)
    guests = range(max(1, group // 2))
    hosts = range(len(guests), group)
    visit = group - 2
    lanes = {(Q, 2): 0, (Q, 3): 1, (K, 0): 2, (V, 0): 2, (K, 2): 2, (V, 2): 2, (K, 3): 2, (V, 3): 2}

    loads = [
        pltpu.make_async_copy(src, given.at[i], load_sem) for i, src in enumerate((q_hbm, k_hbm, v_hbm))
    ]
    table_loads = [
        pltpu.make_async_copy(src, dst, table_sem.at[i])
        for i, (src, dst) in enumerate(((slot_hbm, slot_ref), (table_hbm, table_ref)))
    ]
    past_load = pltpu.make_async_copy(past_hbm, past, past_sem)
    for load in (*loads, past_load, *table_loads):
        load.start()

    def landed(ref, sem):
        pltpu.make_async_copy(ref, ref, sem).wait()

    barrier = pltpu.get_barrier_semaphore()
    for d in (1, 2, 3):
        pl.semaphore_signal(barrier, inc=1, device_id={"uly": peers[d]}, device_id_type=MESH)
    neighbours = {0: (1,), 1: (0, 2, 3), 2: (1, 3), 3: (1, 2)}
    for place, others in neighbours.items():
        @pl.when(s == place)
        def _(place=place, others=others):
            for other in others:
                pl.semaphore_signal(barrier, inc=1, device_id={"seq": other}, device_id_type=MESH)
            if place == 3:
                for d in (1, 2, 3):
                    pl.semaphore_signal(barrier, inc=1, device_id={"seq": 2, "uly": peers[d]}, device_id_type=MESH)
            pl.semaphore_wait(barrier, 3 + len(others) + (3 if place == 2 else 0))
    landed(given, load_sem)

    def columns(uly, g):
        return pl.ds(pl.multiple_of((uly * group + g) * HEAD_DIM, HEAD_DIM), HEAD_DIM)

    def row_range(uly):
        return pl.ds(pl.multiple_of(uly * tokens, tokens), tokens)

    def scatter(kind, g, pieces=None):
        for d in (1, 2, 3, 0):
            src = given.at[kind, :, columns(peers[d], g)]
            dst = heads.at[kind, g, s, row_range(t), :]
            sem = whole_sem.at[kind, g] if pieces is None else piece_sem.at[pieces, d]
            if d == 0:
                pltpu.make_async_copy(src, dst, sem).start()
            else:
                pltpu.make_async_remote_copy(
                    src, dst, plane_send, sem, device_id={"uly": peers[d]}, device_id_type=MESH
                ).start()

    def gathered(kind, g):
        landed(heads.at[kind, g, s], whole_sem.at[kind, g])

    def gathered_piece(kind, g, d, pieces):
        landed(heads.at[kind, g, s, row_range(peers[d]), :], piece_sem.at[pieces, d])

    def arrived(kind, g, block):
        ref = heads.at[Q, g, block] if kind == Q else heads.at[K:V + 1, g, block]
        landed(ref, line_recv.at[lanes[kind, block], g])

    def pass_on(kind, g, d, block, to):
        dst = heads.at[kind, g, block, row_range(peers[d]), :]
        src = given.at[kind, :, columns(t, g)] if d == 0 else dst
        piecewise = kind == Q and block == 3 and g == 1
        if block == 1:
            sem = early_recv.at[1]
        else:
            sem = relay_sem.at[d] if piecewise else line_recv.at[lanes[kind, block], g]
        pltpu.make_async_remote_copy(
            src, dst, line_send.at[kind], sem,
            device_id={"seq": to}, device_id_type=MESH,
        ).start()

    def forward(kind, g, block, to, pieces=None):
        if pieces is None:
            gathered(kind, g)
        for d in (1, 2, 3):
            if pieces is not None:
                gathered_piece(kind, g, d, pieces)
            pass_on(kind, g, d, block, to)

    def relay(g):
        parts = [heads.at[Q, g, 3]]
        if g == 1:
            parts = [heads.at[Q, g, 3, row_range(peers[d]), :] for d in range(n_uly)]
        for d, ref in enumerate(parts):
            landed(ref, relay_sem.at[d] if g == 1 else line_recv.at[lanes[Q, 3], g])
            pltpu.make_async_remote_copy(
                ref, ref, extra_send, line_recv.at[lanes[Q, 3], g], device_id={"seq": 1}, device_id_type=MESH
            ).start()

    def partial(g, where, a, to, slot):
        pltpu.make_async_remote_copy(
            part_out.at[g, where, a], part_in.at[slot, a], part_send, part_recv.at[slot, a],
            device_id={"seq": to}, device_id_type=MESH,
        ).start()

    def give_back(g, ds, lane=0):
        for d in ds:
            src = att.at[lane, g, row_range(peers[d]), :]
            dst = back.at[:, columns(t, g)]
            if lane == 0 and d == 0:
                pltpu.make_async_copy(src, dst, back_sem).start()
                continue
            where = {"uly": peers[d]} if lane == 0 else {"seq": n_seq - 1, "uly": peers[d]}
            pltpu.make_async_remote_copy(
                src, dst, att_send.at[lane], back_sem, device_id=where, device_id_type=MESH
            ).start()

    def attend(g, block, full, diagonal, finish, resume=None):
        query = heads[Q, g, block]
        acc_shape = (rows, HEAD_DIM)
        top = total = acc = None
        if resume is not None:
            top, total, acc = own_stat[resume, 0], own_stat[resume, 1], own[resume]
        for j in (*full, block) if diagonal else full:
            key = heads[K, g, j]
            value = heads[V, g, j]
            scores = lax.dot_general(query, key, (((1,), (1,)), ((), ())), preferred_element_type=jnp.float32)
            scores = scores * scale
            if j == block:
                query_at = lax.broadcasted_iota(jnp.int32, scores.shape, 0)
                key_at = lax.broadcasted_iota(jnp.int32, scores.shape, 1)
                scores = jnp.where(key_at <= query_at, scores, -jnp.inf)
            peak = jnp.broadcast_to(jnp.max(scores, axis=1, keepdims=True), acc_shape)
            new_top = peak if top is None else jnp.maximum(top, peak)
            prob = jnp.exp2(scores - jnp.concatenate([new_top] * (rows // HEAD_DIM), axis=1))
            sums = jnp.broadcast_to(jnp.sum(prob, axis=1, keepdims=True), acc_shape)
            update = jnp.dot(prob.astype(jnp.bfloat16), value, preferred_element_type=jnp.float32)
            if top is None:
                total, acc = sums, update
            else:
                factor = jnp.exp2(top - new_top)
                total = total * factor + sums
                acc = acc * factor + update
            top = new_top
        finish(top, total, acc)

    def settle(g, lane=0):
        def finish(top, total, acc):
            att[lane, g] = (acc / total).astype(jnp.bfloat16)
        return finish

    def keep(slot):
        def finish(top, total, acc):
            own[slot] = acc
            own_stat[slot, 0] = top
            own_stat[slot, 1] = total
        return finish

    def selector(shape, dim, chunk):
        place = lax.broadcasted_iota(jnp.int32, shape, dim) - 3 * chunk
        other = lax.broadcasted_iota(jnp.int32, shape, 1 - dim)
        return place, other

    def packed(top, total):
        level = top + jnp.log2(total)
        high = level.astype(jnp.bfloat16).astype(jnp.float32)
        middle = (level - high).astype(jnp.bfloat16).astype(jnp.float32)
        low = level - high - middle
        lane = lax.broadcasted_iota(jnp.int32, (rows, HEAD_DIM), 1)
        split = jnp.where(lane == 0, high, jnp.where(lane == 1, middle, jnp.where(lane == 2, low, 0.0)))
        return split.astype(jnp.bfloat16)

    def turned(split, first, chunk):
        place, other = selector((STAT, HEAD_DIM), 0, chunk)
        pick = jnp.where((place == other) & (other < 3), 1.0, 0.0).astype(jnp.bfloat16)
        return lax.dot_general(
            pick, split[first:first + HEAD_DIM], (((1,), (1,)), ((), ())), preferred_element_type=jnp.float32
        )

    def level_of(stats, chunk):
        place, _ = selector((STAT, HEAD_DIM), 0, chunk)
        ones = jnp.where((place >= 0) & (place < 3), 1.0, 0.0).astype(jnp.bfloat16)
        return lax.dot_general(stats, ones, (((0,), (0,)), ((), ())), preferred_element_type=jnp.float32)

    def hand_over(g, where):
        def finish(top, total, acc):
            result = (acc / total).astype(jnp.bfloat16)
            split = packed(top, total)
            for a in range(2):
                part_out[g, where, a, 0:half, :] = result[a * half:(a + 1) * half]
                stats = turned(split, a * half, 0) + turned(split, a * half + HEAD_DIM, 1)
                part_out[g, where, a, half:half + STAT, :] = stats.astype(jnp.bfloat16)
        return finish

    def hand_out(where):
        def finish(top, total, acc):
            result = (acc / total).astype(jnp.bfloat16)
            split = packed(top, total)
            for u in range(n_uly):
                last_out[where, u, 0:tokens, :] = result[u * tokens:(u + 1) * tokens]
                last_out[where, u, tokens:tokens + STAT, :] = turned(split, u * tokens, 0).astype(jnp.bfloat16)
        return finish

    def send_last(where, far, block=None):
        for d in (3, 2, 1, 0):
            src, dst = last_out.at[where, peers[d]], last_in.at[1 if far else 0, t]
            if d == 0 and not far:
                pltpu.make_async_copy(src, dst, last_own).start()
                continue
            place = {"uly": peers[d]} if block is None else {"seq": block, "uly": peers[d]}
            pltpu.make_async_remote_copy(
                src, dst, last_send, last_far.at[t] if far else last_own, device_id=place, device_id_type=MESH
            ).start()

    def join_last():
        landed(last_in.at[0], last_own)
        for pair in ((2, 3), (1, 0)):
            for d in pair:
                landed(last_in.at[1, peers[d]], last_far.at[peers[d]])
            for d in pair:
                u = peers[d]
                mine = level_of(last_in[0, u, tokens:tokens + STAT, :], 0)
                theirs = level_of(last_in[1, u, tokens:tokens + STAT, :], 0)
                top = jnp.maximum(mine, theirs)
                mine, theirs = jnp.exp2(mine - top), jnp.exp2(theirs - top)
                first = last_in[0, u, 0:tokens, :].astype(jnp.float32)
                second = last_in[1, u, 0:tokens, :].astype(jnp.float32)
                both = (first * mine + second * theirs) / (mine + theirs)
                back[:, columns(u, group - 1)] = both.astype(jnp.bfloat16)
        landed(back.at[:, 0:(group - 1) * n_uly * HEAD_DIM], back_sem)

    def merge(g, slot, a, lane=0):
        landed(part_in.at[slot, a], part_recv.at[slot, a])
        stats = part_in[slot, a, half:half + STAT, :]
        for chunk in range(2):
            level = level_of(stats, chunk)
            first = pl.multiple_of(a * half + chunk * HEAD_DIM, HEAD_DIM)
            cut = pl.ds(first, HEAD_DIM)
            top, total = own_stat[slot, 0, cut, :], own_stat[slot, 1, cut, :]
            new_top = jnp.maximum(top, level)
            mine, theirs = jnp.exp2(top - new_top), jnp.exp2(level - new_top)
            inverse = 1.0 / (total * mine + theirs)
            other = part_in[slot, a, chunk * HEAD_DIM:(chunk + 1) * HEAD_DIM, :].astype(jnp.float32)
            both = own[slot, cut, :] * (mine * inverse) + other * (theirs * inverse)
            att[lane, g, cut, :] = both.astype(jnp.bfloat16)

    def join(g, slot=None, lane=0):
        slot = g if slot is None else slot
        merge(g, slot, 1 - y, lane)
        give_back(g, (3, 2), lane)
        merge(g, slot, y, lane)
        give_back(g, (1, 0), lane)

    def each(first, count, body):
        def step(g, carry):
            body(g)
            return carry
        lax.fori_loop(first, count, step, 0)

    def add_up():
        for load in (past_load, *table_loads):
            load.wait()
        weights = [table_ref[0, slot_ref[p]] + table_ref[1, slot_ref[p]] for p in range(past.shape[0])]

        def sum_columns(uly):
            cols = pl.ds(pl.multiple_of(uly * (group * HEAD_DIM), HEAD_DIM), group * HEAD_DIM)
            mixed = weights[0] * past[0, :, cols].astype(jnp.float32)
            for p in range(1, past.shape[0]):
                mixed = mixed + weights[p] * past[p, :, cols].astype(jnp.float32)
            base_ref[:, cols] = mixed
        each(0, n_uly, sum_columns)

    def plane_sent():
        landed(given.at[:, :, 0:(n_uly - 1) * group * HEAD_DIM], plane_send)

    def line_sent(kind, block, first=0, count=group):
        landed(heads.at[kind, first:count, block], line_send.at[kind])

    def att_sent(first=0, count=group):
        if count > first:
            landed(att.at[0, first:count, 0:(n_uly - 1) * tokens, :], att_send.at[0])

    @pl.when(s == 0)
    def _():
        order = [(kind, g) for g in range(group) for kind in (K, V)]
        for kind, g in order[:2]:
            pass_on(kind, g, 0, 0, 1)

        @pl.when(ahead)
        def _():
            for kind, g in order[2:4]:
                pass_on(kind, g, 0, 0, 1)
        for i, (kind, g) in enumerate(order):
            scatter(kind, g, i if g == 0 else None)
        for g in range(group):
            scatter(Q, g)
        for i, (kind, g) in enumerate(order):
            if i < 2:
                @pl.when(behind)
                def _(i=i):
                    pass_on(*order[i + 2], 0, 0, 1)
            elif i + 2 < len(order):
                pass_on(*order[i + 2], 0, 0, 1)
            forward(kind, g, 0, 1, i if g == 0 else None)
        for i in range(2):
            gathered_piece(*order[i], 0, i)
        add_up()

        def work(g):
            gathered(Q, g)
            attend(g, 0, (), True, settle(g))
            give_back(g, (3, 2, 1, 0))
        each(0, group, work)
        plane_sent()
        for kind in (K, V):
            line_sent(kind, 0)
        att_sent()
        landed(back, back_sem)

    @pl.when(s == 1)
    def _():
        for kind in (K, V):
            pass_on(kind, 0, 0, 1, 2)
        for i, kind in enumerate((K, V)):
            scatter(kind, 0, i)
        for kind in (K, V):
            scatter(kind, 1)
        scatter(Q, 1)
        scatter(Q, 0)
        for g in range(2, group):
            for kind in (K, V, Q):
                scatter(kind, g)
        for i, kind in enumerate((K, V)):
            forward(kind, 0, 1, 2, i)
            gathered_piece(kind, 0, 0, i)
        add_up()

        def begin(g, block):
            arrived(Q, g, block)
            attend(g, block, (1,), False, keep(block - 2))

        def end(g, block, finish):
            attend(g, block, (0,), False, finish, block - 2)

        def earliest(g):
            arrived(K, g, 0)

        def near(g):
            gathered(Q, g)
            attend(g, 1, (0,), True, settle(g))
            give_back(g, (3, 2, 1, 0))

        def work(g):
            for kind in (K, V):
                gathered(kind, g)
            begin(g, 2)
            earliest(g)
            end(g, 2, hand_over(g, 0))
            for a in (1 - y, y):
                partial(g, 0, a, 2, g)
            begin(g, 3)
            end(g, 3, hand_over(g, 1))
            stays = g < len(guests)
            for a in (1 - y, y):
                partial(g, 1, a, jnp.where(stays, 2, 3), jnp.where(stays, visit + g, g))
            near(g)
        earliest(0)
        for kind in (K, V):
            ref = heads.at[kind, 0, 0]
            pltpu.make_async_remote_copy(
                ref, ref, line_send.at[kind], early_recv.at[0], device_id={"seq": 2}, device_id_type=MESH
            ).start()
        near(0)
        each(1, group - 1, work)
        for kind in (K, V):
            gathered(kind, group - 1)
        begin(group - 1, 3)
        earliest(group - 1)
        end(group - 1, 3, hand_out(1))
        send_last(1, True, 3)
        begin(group - 1, 2)
        end(group - 1, 2, hand_out(0))
        send_last(0, True, 2)
        near(group - 1)
        plane_sent()
        landed(part_out.at[1:], part_send)
        for kind in (K, V):
            landed(heads.at[kind, 0, 0:2], line_send.at[kind])
        landed(last_out, last_send)
        att_sent()
        landed(back, back_sem)

    @pl.when(s == 2)
    def _():
        for kind in (K, V):
            pass_on(kind, hosts[0], 0, 2, 3)
        pass_on(Q, 1, 0, 2, 1)

        @pl.when(ahead)
        def _():
            for g in range(2, group):
                pass_on(Q, g, 0, 2, 1)
        order = [(Q, 1)]
        for g in hosts:
            order += [(K, g), (V, g)] + ([(Q, g)] if g > 1 else [])
        order += [(Q, g) for g in range(2, hosts[0])]
        for kind, g in order:
            scatter(kind, g, g if kind == Q and g < 2 else None)
        scatter(Q, 0)
        for g in guests:
            for kind in (K, V):
                scatter(kind, g)
        for kind, g in order:
            to = 1 if kind == Q else 3
            if kind == Q and g > 1:
                @pl.when(behind)
                def _(g=g):
                    pass_on(Q, g, 0, 2, 1)
            elif kind != Q and g > hosts[0]:
                pass_on(kind, g, 0, 2, 3)
            if kind == Q and g == max(2, group - 1):
                relay(g)
            forward(kind, g, 2, to, g if kind == Q and g < 2 else None)
            if kind == Q and g < max(2, group - 1):
                relay(g)
        gathered_piece(Q, 1, 0, 1)
        add_up()

        def near(g):
            attend(g, 2, (), True, keep(g))

        def own_guest(g):
            for kind in (K, V):
                gathered(kind, g)

        attend(group - 1, 2, (), True, hand_out(0))
        send_last(0, False)
        each(hosts[0], group - 1, near)
        gathered(Q, 0)
        own_guest(0)
        for i in (1, 0):
            landed(heads.at[K:V + 1, 0, i], early_recv.at[i])
        attend(0, 2, (0, 1), True, settle(0))
        give_back(0, (3, 2, 1, 0))
        arrived(Q, 0, 3)
        arrived(K, 0, 3)
        attend(0, 3, (0, 1, 2), True, settle(0, 1))
        give_back(0, (3, 2, 1, 0), 1)
        for g in guests[1:]:
            own_guest(g)
            near(g)
            join(g)
            arrived(K, g, 3)
            attend(g, 3, (2,), True, keep(visit + g))
            join(g, visit + g, 1)
        each(hosts[0], group - 1, join)
        join_last()
        plane_sent()
        line_sent(Q, 2, 1)
        for kind in (K, V):
            line_sent(kind, 2, hosts[0])
        landed(heads.at[Q, 1:, 3], extra_send)
        landed(last_out.at[0, 0:n_uly - 1], last_send)
        landed(att.at[1, 0:len(guests)], att_send.at[1])
        att_sent(0, group - 1)

    @pl.when(s == 3)
    def _():
        order = [(Q, g) for g in (*range(1, group), 0)] + [(kind, g) for g in guests for kind in (K, V)]
        pass_on(Q, 1, 0, 3, 2)

        @pl.when(ahead)
        def _():
            for g in range(2, group):
                pass_on(Q, g, 0, 3, 2)
        for kind, g in order:
            scatter(kind, g, g if kind == Q and g < 2 else None)
        for g in hosts:
            for kind in (K, V):
                scatter(kind, g)
        for kind, g in order:
            if kind != Q or g == 0:
                pass_on(kind, g, 0, 3, 2)
            elif g > 1:
                @pl.when(behind)
                def _(g=g):
                    pass_on(Q, g, 0, 3, 2)
            forward(kind, g, 3, 2, g if kind == Q and g < 2 else None)
        for g in range(2):
            gathered_piece(Q, g, 0, g)
        add_up()

        def near(g, finish=None):
            for kind in (K, V):
                gathered(kind, g)
            arrived(K, g, 2)
            attend(g, 3, (2,), True, keep(g) if finish is None else finish)
        each(hosts[0], group - 1, near)
        near(group - 1, hand_out(0))
        send_last(0, False)
        each(hosts[0], group - 1, join)
        join_last()
        plane_sent()
        line_sent(Q, 3)
        for kind in (K, V):
            line_sent(kind, 3, 0, len(guests))
        landed(last_out.at[0, 0:n_uly - 1], last_send)
        att_sent(hosts[0], group - 1)


def fused(queries, keys, values, past_outputs, dwa_slot, dwa_table):
    n_seq, n_uly = lax.axis_size("seq"), lax.axis_size("uly")
    tokens, features = queries.shape
    group = features // n_uly // HEAD_DIM
    rows = tokens * n_uly
    slots = max(2, group - 2 + max(1, group // 2))
    stored = past_outputs.shape[0]
    bf16, f32 = jnp.bfloat16, jnp.float32
    anywhere = pl.BlockSpec(memory_space=pltpu.HBM)
    attended, base = pl.pallas_call(
        functools.partial(fused_kernel, (n_seq, n_uly, group)),
        out_shape=(pltpu.VMEM((tokens, features), bf16), pltpu.VMEM((tokens, features), f32)),
        in_specs=[anywhere] * 6,
        out_specs=[pl.BlockSpec(memory_space=pltpu.VMEM)] * 2,
        scratch_shapes=[
            pltpu.SMEM(dwa_slot.shape, jnp.int32),
            pltpu.SMEM(dwa_table.shape, f32),
            pltpu.VMEM((3, tokens, features), bf16),
            pltpu.VMEM((stored, tokens, features), bf16),
            pltpu.VMEM((3, group, n_seq, rows, HEAD_DIM), bf16),
            pltpu.VMEM((slots, rows, HEAD_DIM), f32),
            pltpu.VMEM((slots, 2, rows, HEAD_DIM), f32),
            pltpu.VMEM((group - 1, 2, 2, rows // 2 + STAT, HEAD_DIM), bf16),
            pltpu.VMEM((slots, 2, rows // 2 + STAT, HEAD_DIM), bf16),
            pltpu.VMEM((2, group, rows, HEAD_DIM), bf16),
            pltpu.VMEM((2, n_uly, tokens + STAT, HEAD_DIM), bf16),
            pltpu.VMEM((2, n_uly, tokens + STAT, HEAD_DIM), bf16),
            pltpu.SemaphoreType.DMA,
            pltpu.SemaphoreType.DMA,
            pltpu.SemaphoreType.DMA((2,)),
            pltpu.SemaphoreType.DMA,
            pltpu.SemaphoreType.DMA((2, n_uly)),
            pltpu.SemaphoreType.DMA((n_uly,)),
            pltpu.SemaphoreType.DMA((3, group)),
            pltpu.SemaphoreType.DMA((3,)),
            pltpu.SemaphoreType.DMA,
            pltpu.SemaphoreType.DMA((3, group)),
            pltpu.SemaphoreType.DMA((2,)),
            pltpu.SemaphoreType.DMA,
            pltpu.SemaphoreType.DMA((slots, 2)),
            pltpu.SemaphoreType.DMA((2,)),
            pltpu.SemaphoreType.DMA,
            pltpu.SemaphoreType.DMA,
            pltpu.SemaphoreType.DMA,
            pltpu.SemaphoreType.DMA((n_uly,)),
        ],
        compiler_params=pltpu.CompilerParams(
            collective_id=0, has_side_effects=True, vmem_limit_bytes=32 * 1024 * 1024
        ),
    )(*(pltpu.with_memory_space_constraint(x, pltpu.HBM) for x in (dwa_slot, dwa_table, queries, keys, values, past_outputs)))
    return (base + attended.astype(f32)).astype(bf16)


def solution(mesh):
    def body(queries, *rest):
        heads_here = queries.shape[1] // HEAD_DIM // mesh.shape["uly"]
        fits = mesh.shape["seq"] == SPAN and mesh.shape["uly"] == PLANE and heads_here >= 2
        return (fused if fits else shards)(queries, *rest)

    return jax.shard_map(
        body,
        mesh=mesh,
        in_specs=(
            P(("rep", "seq", "uly"), None),
            P(("rep", "seq", "uly"), None),
            P(("rep", "seq", "uly"), None),
            P(None, ("rep", "seq", "uly"), None),
            P(),
            P(),
        ),
        out_specs=P(("rep", "seq", "uly"), None),
        check_vma=False,
    )
```
